8 devices in a mesh: dp: 2 (over z, y), dcp: 4 (over x, core).
Axes of the slice: x: 2, y: 2, z: 1, core: 2. Of those that a mesh axis runs over, the one named last changes fastest.
Arguments:
- q_abs: bfloat16 [256, 64, 576], P('dp', 'dcp'), parts along dimension 0
- latent_cache: bfloat16 [256, 4, 4, 256, 576], P('dp', None, 'dcp'), parts along dimension 0
- ctx_len: int32 [256], P('dp'), parts along dimension 0
Outputs:
- output: bfloat16 [256, 64, 512], P(('dp', 'dcp')), parts along dimension 0
There are 2 independent parts. The reference program is written for one: setup_inputs(seed, part) draws one part's arguments, and reference() takes and returns one part's arrays. A program takes and returns all parts, laid end to end along the dimension named above; each array names one.
All inputs are finite; a program needn't handle non-finite values.
Results may differ from the reference program's by a relative error of at most 0.00722076.
Values are sent between devices in bfloat16 or wider.
A program may use at most 1 GiB of HBM per device.

```python
import math
import jax
import jax.numpy as jnp
from jax import lax

BATCH_SIZE = 128
NUM_HEADS = 64
LATENT_DIM = 512
ROPE_DIM = 64
NOPE_DIM = 128
PAGES_DEV = 4
GROUP_SIZE = 4
PAGE_LEN = 256

WIDTH = LATENT_DIM + ROPE_DIM
SEQ_LEN = PAGES_DEV * GROUP_SIZE * PAGE_LEN


def setup_inputs(seed: int = 0, part: int = 0) -> dict:
    part_key = jax.random.fold_in(jax.random.key(seed), part)
    key_query, key_cache, key_len = jax.random.split(part_key, 3)
    qk_dim = NOPE_DIM + ROPE_DIM
    cache_rope = 1.4
    query_latent = math.sqrt(0.95 * qk_dim / LATENT_DIM)
    query_rope = math.sqrt(0.95 * qk_dim / ROPE_DIM) / cache_rope
    is_latent = jnp.arange(WIDTH) < LATENT_DIM
    query_scale = jnp.where(is_latent, query_latent, query_rope)
    cache_scale = jnp.where(is_latent, 1.0, cache_rope)
    queries = jax.random.normal(key_query, (BATCH_SIZE, NUM_HEADS, WIDTH), jnp.float32) * query_scale
    cache_vals = jax.random.normal(key_cache, (BATCH_SIZE, PAGES_DEV, GROUP_SIZE, PAGE_LEN, WIDTH), jnp.float32) * cache_scale
    len_drop = jax.random.randint(key_len, (BATCH_SIZE,), 0, SEQ_LEN // 2)
    lengths = jnp.where(jnp.arange(BATCH_SIZE) == 0, SEQ_LEN, SEQ_LEN - len_drop)
    return {'q_abs': queries.astype(jnp.bfloat16), 'latent_cache': cache_vals.astype(jnp.bfloat16), 'ctx_len': lengths.astype(jnp.int32)}


def reference(q_abs, latent_cache, ctx_len):
    inv_scale = (NOPE_DIM + ROPE_DIM) ** -0.5
    q_float = q_abs.astype(jnp.float32)
    per_device = jnp.moveaxis(latent_cache, 2, 0)
    page_base = jnp.arange(PAGES_DEV)[:, None] * (GROUP_SIZE * PAGE_LEN) + jnp.arange(PAGE_LEN)[None, :]

    def one_device(carry_in):
        dev_index, cache_blk = carry_in
        cache_float = cache_blk.astype(jnp.float32)
        scores = jnp.einsum('bhw,bjtw->bhjt', q_float, cache_float) * inv_scale
        positions = page_base + dev_index * PAGE_LEN
        is_valid = positions[None, :, :] < ctx_len[:, None, None]
        scores = jnp.where(is_valid[:, None, :, :], scores, -1e30)
        row_max = jnp.max(scores, axis=(2, 3))
        weights_exp = jnp.exp(scores - row_max[:, :, None, None])
        denom_sum = jnp.sum(weights_exp, axis=(2, 3))
        weights_low = weights_exp.astype(jnp.bfloat16).astype(jnp.float32)
        pv_sum = jnp.einsum('bhjt,bjtc->bhc', weights_low, cache_float[..., :LATENT_DIM])
        part_out = (pv_sum / denom_sum[:, :, None]).astype(jnp.bfloat16)
        part_lse = row_max + jnp.log(denom_sum)
        return part_out, part_lse

    part_outs, part_lses = lax.map(one_device, (jnp.arange(GROUP_SIZE), per_device))
    total_lse = jax.nn.logsumexp(part_lses, axis=0)
    merge_weights = jnp.exp(part_lses - total_lse[None])
    merged = jnp.sum(merge_weights[..., None] * part_outs.astype(jnp.float32), axis=0)
    return merged.astype(jnp.bfloat16)
```

```python
import functools
import math

import jax
import jax.numpy as jnp
from jax import lax
from jax.experimental import pallas as pl
from jax.experimental.pallas import tpu as pltpu
from jax.sharding import PartitionSpec as P

ROPE_DIM = 64
QK_DIM = 192
GROUP = 4
CHUNK = 8
PAIR = 2
SLOTS = 3


def attend(q, cache, base, length):
    num_pages, width, page_len = cache.shape
    latent = width - ROPE_DIM
    scores = []
    for j in range(num_pages):
        page = jnp.dot(q, cache[j], preferred_element_type=jnp.float32)
        if j >= num_pages // 2:
            lane = lax.broadcasted_iota(jnp.int32, (1, page_len), 1)
            page = jnp.where(lane < length - (j * GROUP + base) * page_len, page, -jnp.inf)
        scores.append(page)
    top = jnp.max(functools.reduce(jnp.maximum, scores), axis=1, keepdims=True)
    scale = QK_DIM**-0.5
    weights = [jnp.exp2((page - top) * (scale * math.log2(math.e))) for page in scores]
    total = jnp.sum(functools.reduce(jnp.add, weights), axis=1, keepdims=True)
    mixed = functools.reduce(jnp.add, [
        lax.dot_general(weights[j].astype(jnp.bfloat16), cache[j, :latent], (((1,), (1,)), ((), ())),
                        preferred_element_type=jnp.float32) for j in range(num_pages)])
    return (mixed / total).astype(jnp.bfloat16), top * scale + jnp.log(total)


def kernel(q_hbm, cache_hbm, len_ref, out_hbm, q_all, ring, o_buf, o_recv, lse_buf, lse_recv, out_buf,
           own_sem, ring_sem, xs_sem, xr_sem, ds_sem, dr_sem, rs_sem, rr_sem, os_sem, or_sem, ls_sem, lr_sem, out_sem):
    rows, heads, width = q_hbm.shape
    latent = width - ROPE_DIM
    num_chunks = rows // CHUNK
    quarter = num_chunks // GROUP
    steps = rows // PAIR
    per_chunk = CHUNK // PAIR
    me = lax.axis_index("dcp")
    chip = me // 2
    core = me % 2
    across = (me + 2) % GROUP
    sibling = chip * 2 + (1 - core)
    diagonal = (sibling + 2) % GROUP
    first = (1 - chip) * (rows // 2)

    def start_row(k):
        return pl.multiple_of((first + k * CHUNK) % rows, CHUNK)

    def fetch(step):
        row = (first + step * PAIR) % rows
        slot = step % SLOTS
        return pltpu.make_async_copy(cache_hbm.at[pl.ds(row, PAIR), :, 0], ring.at[slot], ring_sem.at[slot])

    def send(src, dst, ssem, rsem, device):
        return pltpu.make_async_remote_copy(src_ref=src, dst_ref=dst, send_sem=ssem, recv_sem=rsem,
                                            device_id={"dcp": device}, device_id_type=pl.DeviceIdType.MESH)

    def send_across(k):
        row = pl.ds(pl.multiple_of((chip * (rows // 2) + k * CHUNK) % rows, CHUNK), CHUNK)
        return send(q_hbm.at[row], q_all.at[me, row], xs_sem.at[k], xr_sem.at[k], across)

    def got_across(k):
        row = pl.ds(start_row(k), CHUNK)
        return send(q_hbm.at[row], q_all.at[across, row], xs_sem.at[k], xr_sem.at[k], across)

    def send_sibling(k):
        row = pl.ds(start_row(k), CHUNK)
        return send(q_hbm.at[row], q_all.at[me, row], ds_sem.at[k], dr_sem.at[k], sibling)

    def got_sibling(k):
        row = pl.ds(start_row(k), CHUNK)
        return send(q_hbm.at[row], q_all.at[sibling, row], ds_sem.at[k], dr_sem.at[k], sibling)

    def relay(k):
        row = pl.ds(start_row(k), CHUNK)
        return send(q_all.at[across, row], q_all.at[across, row], rs_sem.at[k], rr_sem.at[k], sibling)

    def got_relay(k):
        row = pl.ds(start_row(k), CHUNK)
        return send(q_all.at[across, row], q_all.at[diagonal, row], rs_sem.at[k], rr_sem.at[k], sibling)

    def send_part(g, slot, device):
        k = g % quarter
        return (send(o_buf.at[pl.ds(pl.multiple_of(g * CHUNK, CHUNK), CHUNK)], o_recv.at[slot, k],
                     os_sem.at[slot, k], or_sem.at[slot, k], device),
                send(lse_buf.at[g], lse_recv.at[slot, k], ls_sem.at[slot, k], lr_sem.at[slot, k], device))

    own = pltpu.make_async_copy(q_hbm, q_all.at[me], own_sem)
    own.start()
    for step in range(SLOTS - 1):
        fetch(step).start()

    barrier = pltpu.get_barrier_semaphore()
    for device in (across, sibling, diagonal):
        pl.semaphore_signal(barrier, inc=1, device_id={"dcp": device}, device_id_type=pl.DeviceIdType.MESH)
    pl.semaphore_wait(barrier, 3)

    def issue(k, carry):
        send_across(k).start()
        send_sibling(k).start()
        return carry

    lax.fori_loop(0, num_chunks, issue, 0)
    own.wait()
    got_across(0).wait_recv()
    relay(0).start()

    def chunk_step(g, carry):
        @pl.when(g + 1 < num_chunks)
        def _():
            got_across(g + 1).wait_recv()
            relay(g + 1).start()

        got_sibling(g).wait_recv()
        got_relay(g).wait_recv()

        def pair_step(p, lse_acc):
            step = g * per_chunk + p
            fetch(step).wait()

            @pl.when(step + SLOTS - 1 < steps)
            def _():
                fetch(step + SLOTS - 1).start()

            slot = step % SLOTS
            for i in range(PAIR):
                row = (first + step * PAIR + i) % rows
                q = jnp.concatenate([q_all[d, row] for d in range(GROUP)], axis=0)
                o, lse = attend(q, ring[slot, i], me, len_ref[row])
                o_buf[step * PAIR + i] = o
                lane = lax.broadcasted_iota(jnp.int32, lse_acc.shape, 1)
                lse_acc = jnp.where(lane == p * PAIR + i, lse, lse_acc)
            return lse_acc

        lse_acc = lax.fori_loop(0, per_chunk, pair_step, jnp.zeros((GROUP * heads, 128), jnp.float32))
        padded = jnp.concatenate([lse_acc, jnp.zeros((128 - GROUP * heads, 128), jnp.float32)], axis=0)
        lse_buf[g] = padded.T[:CHUNK]

        @pl.when(g < 2 * quarter)
        def _():
            target = (1 - chip) * 2 + g // quarter
            for copy in send_part(g, 1 + (g // quarter + core) % 2, target):
                copy.start()

        @pl.when((g >= 2 * quarter) & (g // quarter - 2 != core))
        def _():
            for copy in send_part(g, 0, sibling):
                copy.start()

        return carry

    lax.fori_loop(0, num_chunks, chunk_step, 0)

    own_first = (2 + core) * quarter

    def merge_step(k, carry):
        for slot in range(GROUP - 1):
            for copy in send_part(k, slot, sibling):
                copy.wait_recv()
        lses = [lse_buf[own_first + k]] + [lse_recv[slot, k] for slot in range(GROUP - 1)]
        top = functools.reduce(jnp.maximum, lses)
        total = top + jnp.log(functools.reduce(jnp.add, [jnp.exp(x - top) for x in lses]))
        factors = jnp.concatenate([jnp.exp(x - total) for x in lses], axis=0)
        padded = jnp.concatenate([factors, jnp.zeros((128 - GROUP * CHUNK, 128), jnp.float32)], axis=0)
        columns = padded.T[:GROUP * heads]
        for i in range(CHUNK):
            parts = [o_buf[(own_first + k) * CHUNK + i]] + [o_recv[slot, k, i] for slot in range(GROUP - 1)]
            merged = functools.reduce(
                jnp.add, [columns[:, s * CHUNK + i:s * CHUNK + i + 1] * part.astype(jnp.float32) for s, part in enumerate(parts)])
            out_buf[k * CHUNK + i] = merged.astype(jnp.bfloat16)
        row = pl.ds(pl.multiple_of(k * CHUNK, CHUNK), CHUNK)
        pltpu.make_async_copy(out_buf.at[row], out_hbm.at[row], out_sem.at[k]).start()
        return carry

    lax.fori_loop(0, quarter, merge_step, 0)

    def drain(k, carry):
        send_across(k).wait_send()
        send_sibling(k).wait_send()
        relay(k).wait_send()
        return carry

    lax.fori_loop(0, num_chunks, drain, 0)
    for k in range(quarter):
        for slot in range(GROUP - 1):
            for copy in send_part(k, slot, sibling):
                copy.wait_send()
        row = pl.ds(k * CHUNK, CHUNK)
        pltpu.make_async_copy(out_buf.at[row], out_hbm.at[row], out_sem.at[k]).wait()


def solution(mesh):
    def local_step(q_blk, cache_blk, len_blk):
        rows, heads, width = q_blk.shape
        num_pages, page_len = cache_blk.shape[1], cache_blk.shape[3]
        cache_blk = jnp.swapaxes(cache_blk, 3, 4)
        latent = width - ROPE_DIM
        num_chunks = rows // CHUNK
        quarter = num_chunks // GROUP
        dma = pltpu.SemaphoreType.DMA
        return pl.pallas_call(
            kernel,
            out_shape=jax.ShapeDtypeStruct((rows // GROUP, GROUP * heads, latent), jnp.bfloat16),
            in_specs=[pl.BlockSpec(memory_space=pl.ANY), pl.BlockSpec(memory_space=pl.ANY),
                      pl.BlockSpec(memory_space=pltpu.SMEM)],
            out_specs=pl.BlockSpec(memory_space=pl.ANY),
            scratch_shapes=[
                pltpu.VMEM((GROUP, rows, heads, width), jnp.bfloat16),
                pltpu.VMEM((SLOTS, PAIR, num_pages, width, page_len), jnp.bfloat16),
                pltpu.VMEM((rows, GROUP * heads, latent), jnp.bfloat16),
                pltpu.VMEM((GROUP - 1, quarter, CHUNK, GROUP * heads, latent), jnp.bfloat16),
                pltpu.VMEM((num_chunks, CHUNK, 128), jnp.float32),
                pltpu.VMEM((GROUP - 1, quarter, CHUNK, 128), jnp.float32),
                pltpu.VMEM((rows // GROUP, GROUP * heads, latent), jnp.bfloat16),
                dma(()), dma((SLOTS,)),
                dma((num_chunks,)), dma((num_chunks,)), dma((num_chunks,)), dma((num_chunks,)),
                dma((num_chunks,)), dma((num_chunks,)),
                dma((GROUP - 1, quarter)), dma((GROUP - 1, quarter)),
                dma((GROUP - 1, quarter)), dma((GROUP - 1, quarter)),
                dma((quarter,)),
            ],
            compiler_params=pltpu.CompilerParams(collective_id=0, has_side_effects=True, vmem_limit_bytes=60 * 2**20),
        )(q_blk, cache_blk, len_blk)

    return jax.shard_map(local_step, mesh=mesh, in_specs=(P('dp', 'dcp', None), P('dp', None, 'dcp', None, None), P('dp')), out_specs=P(('dp', 'dcp'), None, None), check_vma=False)
```

```python
import functools
import math

import jax
import jax.numpy as jnp
from jax import lax
from jax.experimental import pallas as pl
from jax.experimental.pallas import tpu as pltpu
from jax.sharding import PartitionSpec as P

ROPE_DIM = 64
QK_DIM = 192
GROUP = 4
CHUNK = 8
PAIR = 2
SLOTS = 3


def attend(q, q_rope, cache, base, length):
    num_pages, width, page_len = cache.shape
    latent = width - ROPE_DIM
    scores = []
    for j in range(num_pages):
        page = (jnp.dot(q, cache[j, :latent], preferred_element_type=jnp.float32)
                + jnp.dot(q_rope, cache[j, latent:], preferred_element_type=jnp.float32))
        if j >= num_pages // 2:
            lane = lax.broadcasted_iota(jnp.int32, (1, page_len), 1)
            page = jnp.where(lane < length - (j * GROUP + base) * page_len, page, -jnp.inf)
        scores.append(page)
    top = jnp.max(functools.reduce(jnp.maximum, scores), axis=1, keepdims=True)
    scale = QK_DIM**-0.5
    weights = [jnp.exp2((page - top) * (scale * math.log2(math.e))) for page in scores]
    total = jnp.sum(functools.reduce(jnp.add, weights), axis=1, keepdims=True)
    mixed = functools.reduce(jnp.add, [
        lax.dot_general(weights[j].astype(jnp.bfloat16), cache[j, :latent], (((1,), (1,)), ((), ())),
                        preferred_element_type=jnp.float32) for j in range(num_pages)])
    return (mixed / total).astype(jnp.bfloat16), top * scale + jnp.log(total)


def kernel(q_hbm, cache_hbm, len_ref, out_hbm, q_raw, q_turned, q_all, rope_raw, rope_turned, rope_all, ring, o_buf, o_recv, lse_buf, lse_recv, out_buf,
           own_sem, ps_sem, pr_sem, ring_sem, xs_sem, xr_sem, ds_sem, dr_sem, rs_sem, rr_sem, os_sem, or_sem, ls_sem, lr_sem, out_sem):
    heads, width, rows = q_hbm.shape
    latent = width - ROPE_DIM
    num_chunks = rows // CHUNK
    quarter = num_chunks // GROUP
    steps = rows // PAIR
    per_chunk = CHUNK // PAIR
    me = lax.axis_index("dcp")
    chip = me // 2
    core = me % 2
    across = (me + 2) % GROUP
    sibling = chip * 2 + (1 - core)
    diagonal = (sibling + 2) % GROUP
    first = (1 - chip) * (rows // 2)

    def start_row(k):
        return pl.multiple_of((first + k * CHUNK) % rows, CHUNK)

    def fetch(step):
        row = (first + step * PAIR) % rows
        slot = step % SLOTS
        return pltpu.make_async_copy(cache_hbm.at[pl.ds(row, PAIR), :, 0], ring.at[slot], ring_sem.at[slot])

    def send(src, dst, ssem, rsem, device):
        return pltpu.make_async_remote_copy(src_ref=src, dst_ref=dst, send_sem=ssem, recv_sem=rsem,
                                            device_id={"dcp": device}, device_id_type=pl.DeviceIdType.MESH)

    def send_across(k):
        row = pl.ds(pl.multiple_of((chip * (rows // 2) + k * CHUNK) % rows, CHUNK), CHUNK)
        return send(q_all.at[me, row], q_all.at[me, row], xs_sem.at[k], xr_sem.at[k], across)

    def got_across(k):
        row = pl.ds(start_row(k), CHUNK)
        return send(q_all.at[me, row], q_all.at[across, row], xs_sem.at[k], xr_sem.at[k], across)

    def send_sibling(k):
        row = pl.ds(start_row(k), CHUNK)
        return send(q_all.at[me, row], q_all.at[me, row], ds_sem.at[k], dr_sem.at[k], sibling)

    def got_sibling(k):
        row = pl.ds(start_row(k), CHUNK)
        return send(q_all.at[me, row], q_all.at[sibling, row], ds_sem.at[k], dr_sem.at[k], sibling)

    def relay(k):
        row = pl.ds(start_row(k), CHUNK)
        return send(q_all.at[across, row], q_all.at[across, row], rs_sem.at[k], rr_sem.at[k], sibling)

    def got_relay(k):
        row = pl.ds(start_row(k), CHUNK)
        return send(q_all.at[across, row], q_all.at[diagonal, row], rs_sem.at[k], rr_sem.at[k], sibling)

    def send_part(g, slot, device):
        k = g % quarter
        return (send(o_buf.at[pl.ds(pl.multiple_of(g * CHUNK, CHUNK), CHUNK)], o_recv.at[slot, k],
                     os_sem.at[slot, k], or_sem.at[slot, k], device),
                send(lse_buf.at[g], lse_recv.at[slot, k], ls_sem.at[slot, k], lr_sem.at[slot, k], device))

    def send_rope(i, src, dst, device):
        return send(src, rope_raw.at[dst], ps_sem.at[i], pr_sem.at[i], device)

    own_rope = q_hbm.at[:, pl.ds(latent, ROPE_DIM), :]
    own = [pltpu.make_async_copy(q_hbm.at[:, pl.ds(0, latent), :], q_raw, own_sem.at[0]),
           pltpu.make_async_copy(own_rope, rope_raw.at[me], own_sem.at[1])]
    for copy in own:
        copy.start()
    for step in range(SLOTS - 1):
        fetch(step).start()

    barrier = pltpu.get_barrier_semaphore()
    for device in (across, sibling, diagonal):
        pl.semaphore_signal(barrier, inc=1, device_id={"dcp": device}, device_id_type=pl.DeviceIdType.MESH)
    pl.semaphore_wait(barrier, 3)

    send_rope(0, own_rope, me, across).start()
    send_rope(1, own_rope, me, sibling).start()

    block = heads * heads
    into = lax.broadcasted_iota(jnp.int32, (block, block), 0)
    out_of = lax.broadcasted_iota(jnp.int32, (block, block), 1)
    swap = jnp.where(out_of == (into % heads) * heads + into // heads, 1.0, 0.0).astype(jnp.bfloat16)

    def interleave(turned, i):
        part = turned[:, pl.ds(pl.multiple_of(i * heads, heads), heads), :]
        lanes = part.shape[2]
        mixed = jnp.dot(swap, part.reshape(block, lanes), preferred_element_type=jnp.float32)
        return mixed.astype(jnp.bfloat16).reshape(heads, heads, lanes)

    own[0].wait()

    def turn(h, carry):
        q_turned[h] = q_raw[h].T
        return carry

    lax.fori_loop(0, heads, turn, 0)

    def place(i, carry):
        q_all[me, pl.ds(pl.multiple_of(i * heads, heads), heads)] = interleave(q_turned, i)
        return carry

    lax.fori_loop(0, rows // heads, place, 0)

    def issue(k, carry):
        send_across(k).start()
        send_sibling(k).start()
        return carry

    lax.fori_loop(0, num_chunks, issue, 0)
    send_rope(0, own_rope, across, across).wait_recv()
    send_rope(2, rope_raw.at[across], across, sibling).start()
    own[1].wait()
    send_rope(1, own_rope, sibling, sibling).wait_recv()
    send_rope(2, rope_raw.at[across], diagonal, sibling).wait_recv()

    def turn_rope(h, carry):
        rope_turned[h] = jnp.concatenate(
            [jnp.concatenate([rope_raw[d, h], rope_raw[d + 1, h]], axis=0).T for d in range(0, GROUP, 2)], axis=1)
        return carry

    lax.fori_loop(0, heads, turn_rope, 0)

    def place_rope(i, carry):
        rope_all[pl.ds(pl.multiple_of(i * heads, heads), heads)] = interleave(rope_turned, i)
        return carry

    lax.fori_loop(0, rows // heads, place_rope, 0)
    got_across(0).wait_recv()
    relay(0).start()

    def chunk_step(g, carry):
        @pl.when(g + 1 < num_chunks)
        def _():
            got_across(g + 1).wait_recv()
            relay(g + 1).start()

        got_sibling(g).wait_recv()
        got_relay(g).wait_recv()

        def pair_step(p, lse_acc):
            step = g * per_chunk + p
            fetch(step).wait()

            @pl.when(step + SLOTS - 1 < steps)
            def _():
                fetch(step + SLOTS - 1).start()

            slot = step % SLOTS
            for i in range(PAIR):
                row = (first + step * PAIR + i) % rows
                q = jnp.concatenate([q_all[d, row] for d in range(GROUP)], axis=0)
                rope = rope_all[row]
                q_rope = jnp.concatenate([rope[:, d * ROPE_DIM:(d + 1) * ROPE_DIM] for d in range(GROUP)], axis=0)
                o, lse = attend(q, q_rope, ring[slot, i], me, len_ref[row])
                o_buf[step * PAIR + i] = o
                lane = lax.broadcasted_iota(jnp.int32, lse_acc.shape, 1)
                lse_acc = jnp.where(lane == p * PAIR + i, lse, lse_acc)
            return lse_acc

        lse_acc = lax.fori_loop(0, per_chunk, pair_step, jnp.zeros((GROUP * heads, 128), jnp.float32))
        padded = jnp.concatenate([lse_acc, jnp.zeros((128 - GROUP * heads, 128), jnp.float32)], axis=0)
        lse_buf[g] = padded.T[:CHUNK]

        @pl.when(g < 2 * quarter)
        def _():
            target = (1 - chip) * 2 + g // quarter
            for copy in send_part(g, 1 + (g // quarter + core) % 2, target):
                copy.start()

        @pl.when((g >= 2 * quarter) & (g // quarter - 2 != core))
        def _():
            for copy in send_part(g, 0, sibling):
                copy.start()

        return carry

    lax.fori_loop(0, num_chunks, chunk_step, 0)

    own_first = (2 + core) * quarter

    def merge_step(k, carry):
        for slot in range(GROUP - 1):
            for copy in send_part(k, slot, sibling):
                copy.wait_recv()
        lses = [lse_buf[own_first + k]] + [lse_recv[slot, k] for slot in range(GROUP - 1)]
        top = functools.reduce(jnp.maximum, lses)
        total = top + jnp.log(functools.reduce(jnp.add, [jnp.exp(x - top) for x in lses]))
        factors = jnp.concatenate([jnp.exp(x - total) for x in lses], axis=0)
        padded = jnp.concatenate([factors, jnp.zeros((128 - GROUP * CHUNK, 128), jnp.float32)], axis=0)
        columns = padded.T[:GROUP * heads]
        for i in range(CHUNK):
            parts = [o_buf[(own_first + k) * CHUNK + i]] + [o_recv[slot, k, i] for slot in range(GROUP - 1)]
            merged = functools.reduce(
                jnp.add, [columns[:, s * CHUNK + i:s * CHUNK + i + 1] * part.astype(jnp.float32) for s, part in enumerate(parts)])
            out_buf[k * CHUNK + i] = merged.astype(jnp.bfloat16)
        row = pl.ds(pl.multiple_of(k * CHUNK, CHUNK), CHUNK)
        pltpu.make_async_copy(out_buf.at[row], out_hbm.at[row], out_sem.at[k]).start()
        return carry

    lax.fori_loop(0, quarter, merge_step, 0)

    def drain(k, carry):
        send_across(k).wait_send()
        send_sibling(k).wait_send()
        relay(k).wait_send()
        return carry

    lax.fori_loop(0, num_chunks, drain, 0)
    send_rope(0, own_rope, me, across).wait_send()
    send_rope(1, own_rope, me, sibling).wait_send()
    send_rope(2, rope_raw.at[across], across, sibling).wait_send()
    for k in range(quarter):
        for slot in range(GROUP - 1):
            for copy in send_part(k, slot, sibling):
                copy.wait_send()
        row = pl.ds(k * CHUNK, CHUNK)
        pltpu.make_async_copy(out_buf.at[row], out_hbm.at[row], out_sem.at[k]).wait()


def solution(mesh):
    def local_step(q_blk, cache_blk, len_blk):
        rows, heads, width = q_blk.shape
        num_pages, page_len = cache_blk.shape[1], cache_blk.shape[3]
        cache_blk = jnp.swapaxes(cache_blk, 3, 4)
        latent = width - ROPE_DIM
        num_chunks = rows // CHUNK
        quarter = num_chunks // GROUP
        q_blk = jnp.transpose(q_blk, (1, 2, 0))
        dma = pltpu.SemaphoreType.DMA
        return pl.pallas_call(
            kernel,
            out_shape=jax.ShapeDtypeStruct((rows // GROUP, GROUP * heads, latent), jnp.bfloat16),
            in_specs=[pl.BlockSpec(memory_space=pl.ANY), pl.BlockSpec(memory_space=pl.ANY),
                      pl.BlockSpec(memory_space=pltpu.SMEM)],
            out_specs=pl.BlockSpec(memory_space=pl.ANY),
            scratch_shapes=[
                pltpu.VMEM((heads, latent, rows), jnp.bfloat16),
                pltpu.VMEM((heads, rows, latent), jnp.bfloat16),
                pltpu.VMEM((GROUP, rows, heads, latent), jnp.bfloat16),
                pltpu.VMEM((GROUP, heads, ROPE_DIM, rows), jnp.bfloat16),
                pltpu.VMEM((heads, rows, GROUP * ROPE_DIM), jnp.bfloat16),
                pltpu.VMEM((rows, heads, GROUP * ROPE_DIM), jnp.bfloat16),
                pltpu.VMEM((SLOTS, PAIR, num_pages, width, page_len), jnp.bfloat16),
                pltpu.VMEM((rows, GROUP * heads, latent), jnp.bfloat16),
                pltpu.VMEM((GROUP - 1, quarter, CHUNK, GROUP * heads, latent), jnp.bfloat16),
                pltpu.VMEM((num_chunks, CHUNK, 128), jnp.float32),
                pltpu.VMEM((GROUP - 1, quarter, CHUNK, 128), jnp.float32),
                pltpu.VMEM((rows // GROUP, GROUP * heads, latent), jnp.bfloat16),
                dma((2,)), dma((3,)), dma((3,)), dma((SLOTS,)),
                dma((num_chunks,)), dma((num_chunks,)), dma((num_chunks,)), dma((num_chunks,)),
                dma((num_chunks,)), dma((num_chunks,)),
                dma((GROUP - 1, quarter)), dma((GROUP - 1, quarter)),
                dma((GROUP - 1, quarter)), dma((GROUP - 1, quarter)),
                dma((quarter,)),
            ],
            compiler_params=pltpu.CompilerParams(collective_id=0, has_side_effects=True, vmem_limit_bytes=60 * 2**20),
        )(q_blk, cache_blk, len_blk)

    return jax.shard_map(local_step, mesh=mesh, in_specs=(P('dp', 'dcp', None), P('dp', None, 'dcp', None, None), P('dp')), out_specs=P(('dp', 'dcp'), None, None), check_vma=False)
```

```python
import functools
import math

import jax
import jax.numpy as jnp
from jax import lax
from jax.experimental import pallas as pl
from jax.experimental.pallas import tpu as pltpu
from jax.sharding import PartitionSpec as P

ROPE_DIM = 64
QK_DIM = 192
GROUP = 4
CHUNK = 8
PIECE = 4
PAIR = 2
SLOTS = 3


def attend(q, q_rope, cache, base, length):
    num_pages, width, page_len = cache.shape
    latent = width - ROPE_DIM
    scores = []
    for j in range(num_pages):
        page = (jnp.dot(q, cache[j, :latent], preferred_element_type=jnp.float32)
                + jnp.dot(q_rope, cache[j, latent:], preferred_element_type=jnp.float32))
        if j >= num_pages // 2:
            lane = lax.broadcasted_iota(jnp.int32, (1, page_len), 1)
            page = jnp.where(lane < length - (j * GROUP + base) * page_len, page, -jnp.inf)
        scores.append(page)
    top = jnp.max(functools.reduce(jnp.maximum, scores), axis=1, keepdims=True)
    scale = QK_DIM**-0.5
    weights = [jnp.exp2((page - top) * (scale * math.log2(math.e))) for page in scores]
    total = jnp.sum(functools.reduce(jnp.add, weights), axis=1, keepdims=True)
    mixed = functools.reduce(jnp.add, [
        lax.dot_general(weights[j].astype(jnp.bfloat16), cache[j, :latent], (((1,), (1,)), ((), ())),
                        preferred_element_type=jnp.float32) for j in range(num_pages)])
    return (mixed / total).astype(jnp.bfloat16), top * scale + jnp.log(total)


def kernel(q_hbm, cache_hbm, len_ref, out_ref, q_raw, q_turned, q_all, rope_raw, rope_turned, rope_all, ring, o_buf, o_recv, lse_buf, lse_recv,
           own_sem, ps_sem, pr_sem, ring_sem, xs_sem, xr_sem, ds_sem, dr_sem, rs_sem, rr_sem, os_sem, or_sem, ls_sem, lr_sem):
    heads, width, rows = q_hbm.shape
    latent = width - ROPE_DIM
    num_chunks = rows // CHUNK
    quarter = num_chunks // GROUP
    steps = rows // PAIR
    per_chunk = CHUNK // PAIR
    me = lax.axis_index("dcp")
    chip = me // 2
    core = me % 2
    across = (me + 2) % GROUP
    sibling = chip * 2 + (1 - core)
    diagonal = (sibling + 2) % GROUP
    first = (1 - chip) * (rows // 2)

    def start_row(k):
        return pl.multiple_of((first + k * CHUNK) % rows, CHUNK)

    def fetch(step):
        row = (first + step * PAIR) % rows
        slot = step % SLOTS
        return pltpu.make_async_copy(cache_hbm.at[pl.ds(row, PAIR), :, 0], ring.at[slot], ring_sem.at[slot])

    def send(src, dst, ssem, rsem, device):
        return pltpu.make_async_remote_copy(src_ref=src, dst_ref=dst, send_sem=ssem, recv_sem=rsem,
                                            device_id={"dcp": device}, device_id_type=pl.DeviceIdType.MESH)

    def send_across(k):
        row = pl.ds(pl.multiple_of((chip * (rows // 2) + k * CHUNK) % rows, CHUNK), CHUNK)
        return send(q_all.at[me, row], q_all.at[me, row], xs_sem.at[k], xr_sem.at[k], across)

    def got_across(k):
        row = pl.ds(start_row(k), CHUNK)
        return send(q_all.at[me, row], q_all.at[across, row], xs_sem.at[k], xr_sem.at[k], across)

    def send_sibling(k):
        row = pl.ds(start_row(k), CHUNK)
        return send(q_all.at[me, row], q_all.at[me, row], ds_sem.at[k], dr_sem.at[k], sibling)

    def got_sibling(k):
        row = pl.ds(start_row(k), CHUNK)
        return send(q_all.at[me, row], q_all.at[sibling, row], ds_sem.at[k], dr_sem.at[k], sibling)

    def relay(k):
        row = pl.ds(start_row(k), CHUNK)
        return send(q_all.at[across, row], q_all.at[across, row], rs_sem.at[k], rr_sem.at[k], sibling)

    def got_relay(k):
        row = pl.ds(start_row(k), CHUNK)
        return send(q_all.at[across, row], q_all.at[diagonal, row], rs_sem.at[k], rr_sem.at[k], sibling)

    def send_part(g, slot, device):
        k = g % quarter
        copies = [send(lse_buf.at[g], lse_recv.at[slot, k], ls_sem.at[slot, k], lr_sem.at[slot, k], device)]
        for i in range(CHUNK // PIECE):
            rows_i = pl.ds(pl.multiple_of(g * CHUNK + i * PIECE, PIECE), PIECE)
            copies.append(send(o_buf.at[rows_i], o_recv.at[slot, k, pl.ds(i * PIECE, PIECE)],
                               os_sem.at[slot, k, i], or_sem.at[slot, k, i], device))
        return copies

    def send_rope(i, src, dst, device):
        return send(src, rope_raw.at[dst], ps_sem.at[i], pr_sem.at[i], device)

    own_rope = q_hbm.at[:, pl.ds(latent, ROPE_DIM), :]
    own = [pltpu.make_async_copy(q_hbm.at[:, pl.ds(0, latent), :], q_raw, own_sem.at[0]),
           pltpu.make_async_copy(own_rope, rope_raw.at[me], own_sem.at[1])]
    for copy in own:
        copy.start()
    for step in range(SLOTS - 1):
        fetch(step).start()

    barrier = pltpu.get_barrier_semaphore()
    for device in (across, sibling, diagonal):
        pl.semaphore_signal(barrier, inc=1, device_id={"dcp": device}, device_id_type=pl.DeviceIdType.MESH)
    pl.semaphore_wait(barrier, 3)

    send_rope(0, own_rope, me, across).start()
    send_rope(1, own_rope, me, sibling).start()

    block = heads * heads
    into = lax.broadcasted_iota(jnp.int32, (block, block), 0)
    out_of = lax.broadcasted_iota(jnp.int32, (block, block), 1)
    swap = jnp.where(out_of == (into % heads) * heads + into // heads, 1.0, 0.0).astype(jnp.bfloat16)

    def interleave(turned, i):
        part = turned[:, pl.ds(pl.multiple_of(i * heads, heads), heads), :]
        lanes = part.shape[2]
        mixed = jnp.dot(swap, part.reshape(block, lanes), preferred_element_type=jnp.float32)
        return mixed.astype(jnp.bfloat16).reshape(heads, heads, lanes)

    own[0].wait()

    def turn(h, carry):
        q_turned[h] = q_raw[h].T
        return carry

    lax.fori_loop(0, heads, turn, 0)

    def place(i, carry):
        q_all[me, pl.ds(pl.multiple_of(i * heads, heads), heads)] = interleave(q_turned, i)
        return carry

    lax.fori_loop(0, rows // heads, place, 0)

    def issue(k, carry):
        send_across(k).start()
        send_sibling(k).start()
        return carry

    lax.fori_loop(0, num_chunks, issue, 0)
    send_rope(0, own_rope, across, across).wait_recv()
    send_rope(2, rope_raw.at[across], across, sibling).start()
    own[1].wait()
    send_rope(1, own_rope, sibling, sibling).wait_recv()
    send_rope(2, rope_raw.at[across], diagonal, sibling).wait_recv()

    def turn_rope(h, carry):
        rope_turned[h] = jnp.concatenate(
            [jnp.concatenate([rope_raw[d, h], rope_raw[d + 1, h]], axis=0).T for d in range(0, GROUP, 2)], axis=1)
        return carry

    lax.fori_loop(0, heads, turn_rope, 0)

    def place_rope(i, carry):
        rope_all[pl.ds(pl.multiple_of(i * heads, heads), heads)] = interleave(rope_turned, i)
        return carry

    lax.fori_loop(0, rows // heads, place_rope, 0)
    got_across(0).wait_recv()
    relay(0).start()

    def chunk_step(g, carry):
        @pl.when(g + 1 < num_chunks)
        def _():
            got_across(g + 1).wait_recv()
            relay(g + 1).start()

        got_sibling(g).wait_recv()
        got_relay(g).wait_recv()

        def pair_step(p, lse_acc):
            step = g * per_chunk + p
            fetch(step).wait()

            @pl.when(step + SLOTS - 1 < steps)
            def _():
                fetch(step + SLOTS - 1).start()

            slot = step % SLOTS
            for i in range(PAIR):
                row = (first + step * PAIR + i) % rows
                q = jnp.concatenate([q_all[d, row] for d in range(GROUP)], axis=0)
                rope = rope_all[row]
                q_rope = jnp.concatenate([rope[:, d * ROPE_DIM:(d + 1) * ROPE_DIM] for d in range(GROUP)], axis=0)
                o, lse = attend(q, q_rope, ring[slot, i], me, len_ref[row])
                o_buf[step * PAIR + i] = o
                lane = lax.broadcasted_iota(jnp.int32, lse_acc.shape, 1)
                lse_acc = jnp.where(lane == p * PAIR + i, lse, lse_acc)
            return lse_acc

        lse_acc = lax.fori_loop(0, per_chunk, pair_step, jnp.zeros((GROUP * heads, 128), jnp.float32))
        padded = jnp.concatenate([lse_acc, jnp.zeros((128 - GROUP * heads, 128), jnp.float32)], axis=0)
        lse_buf[g] = padded.T[:CHUNK]

        @pl.when(g < 2 * quarter)
        def _():
            target = (1 - chip) * 2 + g // quarter
            for copy in send_part(g, 1 + (g // quarter + core) % 2, target):
                copy.start()

        @pl.when((g >= 2 * quarter) & (g // quarter - 2 != core))
        def _():
            for copy in send_part(g, 0, sibling):
                copy.start()

        return carry

    lax.fori_loop(0, num_chunks, chunk_step, 0)

    own_first = (2 + core) * quarter

    def merge_step(k, carry):
        parts_of = [send_part(k, slot, sibling) for slot in range(GROUP - 1)]
        for part in parts_of:
            part[0].wait_recv()
        lses = [lse_buf[own_first + k]] + [lse_recv[slot, k] for slot in range(GROUP - 1)]
        top = functools.reduce(jnp.maximum, lses)
        total = top + jnp.log(functools.reduce(jnp.add, [jnp.exp(x - top) for x in lses]))
        factors = jnp.concatenate([jnp.exp(x - total) for x in lses], axis=0)
        padded = jnp.concatenate([factors, jnp.zeros((128 - GROUP * CHUNK, 128), jnp.float32)], axis=0)
        columns = padded.T[:GROUP * heads]
        for i in range(CHUNK):
            if i % PIECE == 0:
                for part in parts_of:
                    part[1 + i // PIECE].wait_recv()
            parts = [o_buf[(own_first + k) * CHUNK + i]] + [o_recv[slot, k, i] for slot in range(GROUP - 1)]
            merged = functools.reduce(
                jnp.add, [columns[:, s * CHUNK + i:s * CHUNK + i + 1] * part.astype(jnp.float32) for s, part in enumerate(parts)])
            out_ref[k * CHUNK + i] = merged.astype(jnp.bfloat16)
        return carry

    lax.fori_loop(0, quarter, merge_step, 0)

    def drain(k, carry):
        send_across(k).wait_send()
        send_sibling(k).wait_send()
        relay(k).wait_send()
        return carry

    lax.fori_loop(0, num_chunks, drain, 0)
    send_rope(0, own_rope, me, across).wait_send()
    send_rope(1, own_rope, me, sibling).wait_send()
    send_rope(2, rope_raw.at[across], across, sibling).wait_send()
    for k in range(quarter):
        for slot in range(GROUP - 1):
            for copy in send_part(k, slot, sibling):
                copy.wait_send()


def solution(mesh):
    def local_step(q_blk, cache_blk, len_blk):
        rows, heads, width = q_blk.shape
        num_pages, page_len = cache_blk.shape[1], cache_blk.shape[3]
        cache_blk = jnp.swapaxes(cache_blk, 3, 4)
        latent = width - ROPE_DIM
        num_chunks = rows // CHUNK
        quarter = num_chunks // GROUP
        q_blk = jnp.transpose(q_blk, (1, 2, 0))
        dma = pltpu.SemaphoreType.DMA
        return pl.pallas_call(
            kernel,
            out_shape=pltpu.VMEM((rows // GROUP, GROUP * heads, latent), jnp.bfloat16),
            in_specs=[pl.BlockSpec(memory_space=pl.ANY), pl.BlockSpec(memory_space=pl.ANY),
                      pl.BlockSpec(memory_space=pltpu.SMEM)],
            out_specs=pl.BlockSpec(memory_space=pltpu.VMEM),
            scratch_shapes=[
                pltpu.VMEM((heads, latent, rows), jnp.bfloat16),
                pltpu.VMEM((heads, rows, latent), jnp.bfloat16),
                pltpu.VMEM((GROUP, rows, heads, latent), jnp.bfloat16),
                pltpu.VMEM((GROUP, heads, ROPE_DIM, rows), jnp.bfloat16),
                pltpu.VMEM((heads, rows, GROUP * ROPE_DIM), jnp.bfloat16),
                pltpu.VMEM((rows, heads, GROUP * ROPE_DIM), jnp.bfloat16),
                pltpu.VMEM((SLOTS, PAIR, num_pages, width, page_len), jnp.bfloat16),
                pltpu.VMEM((rows, GROUP * heads, latent), jnp.bfloat16),
                pltpu.VMEM((GROUP - 1, quarter, CHUNK, GROUP * heads, latent), jnp.bfloat16),
                pltpu.VMEM((num_chunks, CHUNK, 128), jnp.float32),
                pltpu.VMEM((GROUP - 1, quarter, CHUNK, 128), jnp.float32),
                dma((2,)), dma((3,)), dma((3,)), dma((SLOTS,)),
                dma((num_chunks,)), dma((num_chunks,)), dma((num_chunks,)), dma((num_chunks,)),
                dma((num_chunks,)), dma((num_chunks,)),
                dma((GROUP - 1, quarter, CHUNK // PIECE)), dma((GROUP - 1, quarter, CHUNK // PIECE)),
                dma((GROUP - 1, quarter)), dma((GROUP - 1, quarter)),
            ],
            compiler_params=pltpu.CompilerParams(collective_id=0, has_side_effects=True, vmem_limit_bytes=60 * 2**20),
        )(q_blk, cache_blk, len_blk)

    return jax.shard_map(local_step, mesh=mesh, in_specs=(P('dp', 'dcp', None), P('dp', None, 'dcp', None, None), P('dp')), out_specs=P(('dp', 'dcp'), None, None), check_vma=False)
```

```python
import functools
import math

import jax
import jax.numpy as jnp
from jax import lax
from jax.experimental import pallas as pl
from jax.experimental.pallas import tpu as pltpu
from jax.sharding import PartitionSpec as P

ROPE_DIM = 64
QK_DIM = 192
GROUP = 4
CHUNK = 8
PIECE = 4
PAIR = 2
SLOTS = 3


def attend(q, q_rope, cache, base, length):
    num_pages, width, page_len = cache.shape
    latent = width - ROPE_DIM
    scores = []
    for j in range(num_pages):
        page = (jnp.dot(q, cache[j, :latent], preferred_element_type=jnp.float32)
                + jnp.dot(q_rope, cache[j, latent:], preferred_element_type=jnp.float32))
        if j >= num_pages // 2:
            lane = lax.broadcasted_iota(jnp.int32, (1, page_len), 1)
            page = jnp.where(lane < length - (j * GROUP + base) * page_len, page, -jnp.inf)
        scores.append(page)
    top = jnp.max(functools.reduce(jnp.maximum, scores), axis=1, keepdims=True)
    scale = QK_DIM**-0.5
    weights = [jnp.exp2((page - top) * (scale * math.log2(math.e))) for page in scores]
    total = jnp.sum(functools.reduce(jnp.add, weights), axis=1, keepdims=True)
    mixed = functools.reduce(jnp.add, [
        lax.dot_general(weights[j].astype(jnp.bfloat16), cache[j, :latent], (((1,), (1,)), ((), ())),
                        preferred_element_type=jnp.float32) for j in range(num_pages)])
    return (mixed / total).astype(jnp.bfloat16), top * scale + jnp.log(total)


def kernel(q_hbm, cache_hbm, len_ref, out_ref, q_raw, q_turned, q_all, rope_raw, rope_turned, rope_all, ring, o_buf, o_recv, lse_buf, lse_recv,
           own_sem, ps_sem, pr_sem, ring_sem, xs_sem, xr_sem, ds_sem, dr_sem, rs_sem, rr_sem, os_sem, or_sem, ls_sem, lr_sem, ready):
    heads, width, rows = q_hbm.shape
    latent = width - ROPE_DIM
    num_chunks = rows // CHUNK
    quarter = num_chunks // GROUP
    steps = rows // PAIR
    per_chunk = CHUNK // PAIR
    me = lax.axis_index("dcp")
    chip = me // 2
    core = me % 2
    across = (me + 2) % GROUP
    sibling = chip * 2 + (1 - core)
    diagonal = (sibling + 2) % GROUP
    first = (1 - chip) * (rows // 2)

    def start_row(k):
        return pl.multiple_of((first + k * CHUNK) % rows, CHUNK)

    def fetch(step):
        row = (first + step * PAIR) % rows
        slot = step % SLOTS
        return pltpu.make_async_copy(cache_hbm.at[pl.ds(row, PAIR), :, 0], ring.at[slot], ring_sem.at[slot])

    def send(src, dst, ssem, rsem, device):
        return pltpu.make_async_remote_copy(src_ref=src, dst_ref=dst, send_sem=ssem, recv_sem=rsem,
                                            device_id={"dcp": device}, device_id_type=pl.DeviceIdType.MESH)

    def send_across(k):
        row = pl.ds(pl.multiple_of((chip * (rows // 2) + k * CHUNK) % rows, CHUNK), CHUNK)
        return send(q_all.at[me, row], q_all.at[me, row], xs_sem.at[k], xr_sem.at[k], across)

    def got_across(k):
        row = pl.ds(start_row(k), CHUNK)
        return send(q_all.at[me, row], q_all.at[across, row], xs_sem.at[k], xr_sem.at[k], across)

    def send_sibling(k):
        row = pl.ds(start_row(k), CHUNK)
        return send(q_all.at[me, row], q_all.at[me, row], ds_sem.at[k], dr_sem.at[k], sibling)

    def got_sibling(k):
        row = pl.ds(start_row(k), CHUNK)
        return send(q_all.at[me, row], q_all.at[sibling, row], ds_sem.at[k], dr_sem.at[k], sibling)

    def relay(k):
        row = pl.ds(start_row(k), CHUNK)
        return send(q_all.at[across, row], q_all.at[across, row], rs_sem.at[k], rr_sem.at[k], sibling)

    def got_relay(k):
        row = pl.ds(start_row(k), CHUNK)
        return send(q_all.at[across, row], q_all.at[diagonal, row], rs_sem.at[k], rr_sem.at[k], sibling)

    def send_part(g, slot, device):
        k = g % quarter
        copies = [send(lse_buf.at[g], lse_recv.at[slot, k], ls_sem.at[slot, k], lr_sem.at[slot, k], device)]
        for i in range(CHUNK // PIECE):
            rows_i = pl.ds(pl.multiple_of(g * CHUNK + i * PIECE, PIECE), PIECE)
            copies.append(send(o_buf.at[rows_i], o_recv.at[slot, k, pl.ds(i * PIECE, PIECE)],
                               os_sem.at[slot, k, i], or_sem.at[slot, k, i], device))
        return copies

    def send_rope(i, src, dst, device):
        return send(src, rope_raw.at[dst], ps_sem.at[i], pr_sem.at[i], device)

    own_rope = q_hbm.at[:, pl.ds(latent, ROPE_DIM), :]
    own = [pltpu.make_async_copy(q_hbm.at[:, pl.ds(0, latent), :], q_raw, own_sem.at[0]),
           pltpu.make_async_copy(own_rope, rope_raw.at[me], own_sem.at[1])]
    for copy in own:
        copy.start()
    for step in range(SLOTS - 1):
        fetch(step).start()

    def tell(semaphore, device):
        pl.semaphore_signal(semaphore, inc=1, device_id={"dcp": device}, device_id_type=pl.DeviceIdType.MESH)

    barrier = pltpu.get_barrier_semaphore()
    tell(barrier, across)
    pl.semaphore_wait(barrier, 3 - 2 * core)

    @pl.when(core == 1)
    def _():
        tell(barrier, sibling)
        tell(barrier, diagonal)

    @pl.when(core == 0)
    def _():
        tell(ready, sibling)
        tell(ready, diagonal)

    send_rope(0, own_rope, me, across).start()

    block = heads * heads
    into = lax.broadcasted_iota(jnp.int32, (block, block), 0)
    out_of = lax.broadcasted_iota(jnp.int32, (block, block), 1)
    swap = jnp.where(out_of == (into % heads) * heads + into // heads, 1.0, 0.0).astype(jnp.bfloat16)

    def interleave(turned, i):
        part = turned[:, pl.ds(pl.multiple_of(i * heads, heads), heads), :]
        lanes = part.shape[2]
        mixed = jnp.dot(swap, part.reshape(block, lanes), preferred_element_type=jnp.float32)
        return mixed.astype(jnp.bfloat16).reshape(heads, heads, lanes)

    own[0].wait()

    def turn(h, carry):
        q_turned[h] = q_raw[h].T
        return carry

    lax.fori_loop(0, heads, turn, 0)

    def place(i, carry):
        q_all[me, pl.ds(pl.multiple_of(i * heads, heads), heads)] = interleave(q_turned, i)
        return carry

    lax.fori_loop(0, rows // heads, place, 0)

    def issue_across(k, carry):
        send_across(k).start()
        return carry

    lax.fori_loop(0, num_chunks, issue_across, 0)

    @pl.when(core == 1)
    def _():
        pl.semaphore_wait(ready, 2)

    send_rope(1, own_rope, me, sibling).start()

    def issue_sibling(k, carry):
        send_sibling(k).start()
        return carry

    lax.fori_loop(0, num_chunks, issue_sibling, 0)
    send_rope(0, own_rope, across, across).wait_recv()
    send_rope(2, rope_raw.at[across], across, sibling).start()
    own[1].wait()
    send_rope(1, own_rope, sibling, sibling).wait_recv()
    send_rope(2, rope_raw.at[across], diagonal, sibling).wait_recv()

    def turn_rope(h, carry):
        rope_turned[h] = jnp.concatenate(
            [jnp.concatenate([rope_raw[d, h], rope_raw[d + 1, h]], axis=0).T for d in range(0, GROUP, 2)], axis=1)
        return carry

    lax.fori_loop(0, heads, turn_rope, 0)

    def place_rope(i, carry):
        rope_all[pl.ds(pl.multiple_of(i * heads, heads), heads)] = interleave(rope_turned, i)
        return carry

    lax.fori_loop(0, rows // heads, place_rope, 0)
    got_across(0).wait_recv()
    relay(0).start()

    def chunk_step(g, carry):
        @pl.when(g + 1 < num_chunks)
        def _():
            got_across(g + 1).wait_recv()
            relay(g + 1).start()

        got_sibling(g).wait_recv()
        got_relay(g).wait_recv()

        def pair_step(p, lse_acc):
            step = g * per_chunk + p
            fetch(step).wait()

            @pl.when(step + SLOTS - 1 < steps)
            def _():
                fetch(step + SLOTS - 1).start()

            slot = step % SLOTS
            for i in range(PAIR):
                row = (first + step * PAIR + i) % rows
                q = jnp.concatenate([q_all[d, row] for d in range(GROUP)], axis=0)
                rope = rope_all[row]
                q_rope = jnp.concatenate([rope[:, d * ROPE_DIM:(d + 1) * ROPE_DIM] for d in range(GROUP)], axis=0)
                o, lse = attend(q, q_rope, ring[slot, i], me, len_ref[row])
                o_buf[step * PAIR + i] = o
                lane = lax.broadcasted_iota(jnp.int32, lse_acc.shape, 1)
                lse_acc = jnp.where(lane == p * PAIR + i, lse, lse_acc)
            return lse_acc

        lse_acc = lax.fori_loop(0, per_chunk, pair_step, jnp.zeros((GROUP * heads, 128), jnp.float32))
        padded = jnp.concatenate([lse_acc, jnp.zeros((128 - GROUP * heads, 128), jnp.float32)], axis=0)
        lse_buf[g] = padded.T[:CHUNK]

        @pl.when(g < 2 * quarter)
        def _():
            target = (1 - chip) * 2 + g // quarter
            for copy in send_part(g, 1 + (g // quarter + core) % 2, target):
                copy.start()

        @pl.when((g >= 2 * quarter) & (g // quarter - 2 != core))
        def _():
            for copy in send_part(g, 0, sibling):
                copy.start()

        return carry

    lax.fori_loop(0, num_chunks, chunk_step, 0)

    own_first = (2 + core) * quarter

    def merge_step(k, carry):
        parts_of = [send_part(k, slot, sibling) for slot in range(GROUP - 1)]
        for part in parts_of:
            part[0].wait_recv()
        lses = [lse_buf[own_first + k]] + [lse_recv[slot, k] for slot in range(GROUP - 1)]
        top = functools.reduce(jnp.maximum, lses)
        total = top + jnp.log(functools.reduce(jnp.add, [jnp.exp(x - top) for x in lses]))
        factors = jnp.concatenate([jnp.exp(x - total) for x in lses], axis=0)
        padded = jnp.concatenate([factors, jnp.zeros((128 - GROUP * CHUNK, 128), jnp.float32)], axis=0)
        columns = padded.T[:GROUP * heads]
        for i in range(CHUNK):
            if i % PIECE == 0:
                for part in parts_of:
                    part[1 + i // PIECE].wait_recv()
            parts = [o_buf[(own_first + k) * CHUNK + i]] + [o_recv[slot, k, i] for slot in range(GROUP - 1)]
            merged = functools.reduce(
                jnp.add, [columns[:, s * CHUNK + i:s * CHUNK + i + 1] * part.astype(jnp.float32) for s, part in enumerate(parts)])
            out_ref[k * CHUNK + i] = merged.astype(jnp.bfloat16)
        return carry

    lax.fori_loop(0, quarter, merge_step, 0)

    def drain(k, carry):
        send_across(k).wait_send()
        send_sibling(k).wait_send()
        relay(k).wait_send()
        return carry

    lax.fori_loop(0, num_chunks, drain, 0)
    send_rope(0, own_rope, me, across).wait_send()
    send_rope(1, own_rope, me, sibling).wait_send()
    send_rope(2, rope_raw.at[across], across, sibling).wait_send()
    for k in range(quarter):
        for slot in range(GROUP - 1):
            for copy in send_part(k, slot, sibling):
                copy.wait_send()


def solution(mesh):
    def local_step(q_blk, cache_blk, len_blk):
        rows, heads, width = q_blk.shape
        num_pages, page_len = cache_blk.shape[1], cache_blk.shape[3]
        cache_blk = jnp.swapaxes(cache_blk, 3, 4)
        latent = width - ROPE_DIM
        num_chunks = rows // CHUNK
        quarter = num_chunks // GROUP
        q_blk = jnp.transpose(q_blk, (1, 2, 0))
        dma = pltpu.SemaphoreType.DMA
        return pl.pallas_call(
            kernel,
            out_shape=pltpu.VMEM((rows // GROUP, GROUP * heads, latent), jnp.bfloat16),
            in_specs=[pl.BlockSpec(memory_space=pl.ANY), pl.BlockSpec(memory_space=pl.ANY),
                      pl.BlockSpec(memory_space=pltpu.SMEM)],
            out_specs=pl.BlockSpec(memory_space=pltpu.VMEM),
            scratch_shapes=[
                pltpu.VMEM((heads, latent, rows), jnp.bfloat16),
                pltpu.VMEM((heads, rows, latent), jnp.bfloat16),
                pltpu.VMEM((GROUP, rows, heads, latent), jnp.bfloat16),
                pltpu.VMEM((GROUP, heads, ROPE_DIM, rows), jnp.bfloat16),
                pltpu.VMEM((heads, rows, GROUP * ROPE_DIM), jnp.bfloat16),
                pltpu.VMEM((rows, heads, GROUP * ROPE_DIM), jnp.bfloat16),
                pltpu.VMEM((SLOTS, PAIR, num_pages, width, page_len), jnp.bfloat16),
                pltpu.VMEM((rows, GROUP * heads, latent), jnp.bfloat16),
                pltpu.VMEM((GROUP - 1, quarter, CHUNK, GROUP * heads, latent), jnp.bfloat16),
                pltpu.VMEM((num_chunks, CHUNK, 128), jnp.float32),
                pltpu.VMEM((GROUP - 1, quarter, CHUNK, 128), jnp.float32),
                dma((2,)), dma((3,)), dma((3,)), dma((SLOTS,)),
                dma((num_chunks,)), dma((num_chunks,)), dma((num_chunks,)), dma((num_chunks,)),
                dma((num_chunks,)), dma((num_chunks,)),
                dma((GROUP - 1, quarter, CHUNK // PIECE)), dma((GROUP - 1, quarter, CHUNK // PIECE)),
                dma((GROUP - 1, quarter)), dma((GROUP - 1, quarter)),
                pltpu.SemaphoreType.REGULAR,
            ],
            compiler_params=pltpu.CompilerParams(collective_id=0, has_side_effects=True, vmem_limit_bytes=60 * 2**20),
        )(q_blk, cache_blk, len_blk)

    return jax.shard_map(local_step, mesh=mesh, in_specs=(P('dp', 'dcp', None), P('dp', None, 'dcp', None, None), P('dp')), out_specs=P(('dp', 'dcp'), None, None), check_vma=False)
```

```python
import functools
import math

import jax
import jax.numpy as jnp
from jax import lax
from jax.experimental import pallas as pl
from jax.experimental.pallas import tpu as pltpu
from jax.sharding import PartitionSpec as P

ROPE_DIM = 64
QK_DIM = 192
GROUP = 4
CHUNK = 16
PIECES = (8, 4, 2, 2)
PAIR = 2
SLOTS = 3


def attend(q, q_rope, cache, base, length):
    num_pages, width, page_len = cache.shape
    latent = width - ROPE_DIM
    scores = []
    for j in range(num_pages):
        page = (jnp.dot(q, cache[j, :latent], preferred_element_type=jnp.float32)
                + jnp.dot(q_rope, cache[j, latent:], preferred_element_type=jnp.float32))
        if j >= num_pages // 2:
            lane = lax.broadcasted_iota(jnp.int32, (1, page_len), 1)
            page = jnp.where(lane < length - (j * GROUP + base) * page_len, page, -jnp.inf)
        scores.append(page)
    top = jnp.max(functools.reduce(jnp.maximum, scores), axis=1, keepdims=True)
    scale = QK_DIM**-0.5
    weights = [jnp.exp2((page - top) * (scale * math.log2(math.e))) for page in scores]
    total = jnp.sum(functools.reduce(jnp.add, weights), axis=1, keepdims=True)
    mixed = functools.reduce(jnp.add, [
        lax.dot_general(weights[j].astype(jnp.bfloat16), cache[j, :latent], (((1,), (1,)), ((), ())),
                        preferred_element_type=jnp.float32) for j in range(num_pages)])
    return (mixed / total).astype(jnp.bfloat16), top * scale + jnp.log(total)


def kernel(q_hbm, cache_hbm, len_hbm, out_ref, len_ref, q_raw, q_turned, q_all, rope_raw, rope_turned, rope_all, ring, o_buf, o_recv, lse_buf, lse_recv,
           len_sem, own_sem, ps_sem, pr_sem, ring_sem, xs_sem, xr_sem, ds_sem, dr_sem, rs_sem, rr_sem, os_sem, or_sem, ls_sem, lr_sem, ready):
    heads, width, rows = q_hbm.shape
    latent = width - ROPE_DIM
    num_chunks = rows // CHUNK
    quarter = num_chunks // GROUP
    steps = rows // PAIR
    per_chunk = CHUNK // PAIR
    me = lax.axis_index("dcp")
    chip = me // 2
    core = me % 2
    across = (me + 2) % GROUP
    sibling = chip * 2 + (1 - core)
    diagonal = (sibling + 2) % GROUP
    first = (1 - chip) * (rows // 2)

    def start_row(k):
        return pl.multiple_of((first + k * CHUNK) % rows, CHUNK)

    def fetch(step):
        row = (first + step * PAIR) % rows
        slot = step % SLOTS
        return pltpu.make_async_copy(cache_hbm.at[pl.ds(row, PAIR), :, 0], ring.at[slot], ring_sem.at[slot])

    def send(src, dst, ssem, rsem, device):
        return pltpu.make_async_remote_copy(src_ref=src, dst_ref=dst, send_sem=ssem, recv_sem=rsem,
                                            device_id={"dcp": device}, device_id_type=pl.DeviceIdType.MESH)

    def send_across(k):
        row = pl.ds(pl.multiple_of((chip * (rows // 2) + k * CHUNK) % rows, CHUNK), CHUNK)
        return send(q_all.at[me, row], q_all.at[me, row], xs_sem.at[k], xr_sem.at[k], across)

    def got_across(k):
        row = pl.ds(start_row(k), CHUNK)
        return send(q_all.at[me, row], q_all.at[across, row], xs_sem.at[k], xr_sem.at[k], across)

    def send_sibling(k):
        row = pl.ds(start_row(k), CHUNK)
        return send(q_all.at[me, row], q_all.at[me, row], ds_sem.at[k], dr_sem.at[k], sibling)

    def got_sibling(k):
        row = pl.ds(start_row(k), CHUNK)
        return send(q_all.at[me, row], q_all.at[sibling, row], ds_sem.at[k], dr_sem.at[k], sibling)

    def relay(k):
        row = pl.ds(start_row(k), CHUNK)
        return send(q_all.at[across, row], q_all.at[across, row], rs_sem.at[k], rr_sem.at[k], sibling)

    def got_relay(k):
        row = pl.ds(start_row(k), CHUNK)
        return send(q_all.at[across, row], q_all.at[diagonal, row], rs_sem.at[k], rr_sem.at[k], sibling)

    def send_part(g, slot, device):
        k = g % quarter
        copies, begin = [], 0
        for i, size in enumerate(PIECES):
            src = o_buf.at[pl.ds(pl.multiple_of(g * CHUNK + begin, size), size)]
            copies.append(send(src, o_recv.at[slot, k, pl.ds(begin, size)],
                               os_sem.at[slot, k, i], or_sem.at[slot, k, i], device))
            begin += size
        return copies + [send(lse_buf.at[g], lse_recv.at[slot, k], ls_sem.at[slot, k], lr_sem.at[slot, k], device)]

    def send_rope(i, src, dst, device):
        return send(src, rope_raw.at[dst], ps_sem.at[i], pr_sem.at[i], device)

    own_rope = q_hbm.at[:, pl.ds(latent, ROPE_DIM), :]
    own = [pltpu.make_async_copy(q_hbm.at[:, pl.ds(0, latent), :], q_raw, own_sem.at[0]),
           pltpu.make_async_copy(own_rope, rope_raw.at[me], own_sem.at[1])]
    lengths = pltpu.make_async_copy(len_hbm, len_ref, len_sem)
    for copy in own + [lengths]:
        copy.start()
    for step in range(SLOTS - 1):
        fetch(step).start()

    def tell(semaphore, device):
        pl.semaphore_signal(semaphore, inc=1, device_id={"dcp": device}, device_id_type=pl.DeviceIdType.MESH)

    barrier = pltpu.get_barrier_semaphore()
    tell(barrier, across)
    pl.semaphore_wait(barrier, 3 - 2 * core)

    @pl.when(core == 1)
    def _():
        tell(barrier, sibling)
        tell(barrier, diagonal)

    @pl.when(core == 0)
    def _():
        tell(ready, sibling)
        tell(ready, diagonal)

    send_rope(0, own_rope, me, across).start()

    block = heads * heads
    into = lax.broadcasted_iota(jnp.int32, (block, block), 0)
    out_of = lax.broadcasted_iota(jnp.int32, (block, block), 1)
    swap = jnp.where(out_of == (into % heads) * heads + into // heads, 1.0, 0.0).astype(jnp.bfloat16)

    def interleave(turned, i):
        part = turned[:, pl.ds(pl.multiple_of(i * heads, heads), heads), :]
        lanes = part.shape[2]
        mixed = jnp.dot(swap, part.reshape(block, lanes), preferred_element_type=jnp.float32)
        return mixed.astype(jnp.bfloat16).reshape(heads, heads, lanes)

    own[0].wait()

    def turn(h, carry):
        q_turned[h] = q_raw[h].T
        return carry

    lax.fori_loop(0, heads, turn, 0)

    def place(i, carry):
        q_all[me, pl.ds(pl.multiple_of(i * heads, heads), heads)] = interleave(q_turned, i)
        return carry

    lax.fori_loop(0, rows // heads, place, 0)

    def issue_across(k, carry):
        send_across(k).start()
        return carry

    lax.fori_loop(0, num_chunks, issue_across, 0)

    @pl.when(core == 1)
    def _():
        pl.semaphore_wait(ready, 2)

    send_rope(1, own_rope, me, sibling).start()

    def issue_sibling(k, carry):
        send_sibling(k).start()
        return carry

    lax.fori_loop(0, num_chunks, issue_sibling, 0)
    send_rope(0, own_rope, across, across).wait_recv()
    send_rope(2, rope_raw.at[across], across, sibling).start()
    own[1].wait()
    send_rope(1, own_rope, sibling, sibling).wait_recv()
    send_rope(2, rope_raw.at[across], diagonal, sibling).wait_recv()

    def turn_rope(h, carry):
        rope_turned[h] = jnp.concatenate(
            [jnp.concatenate([rope_raw[d, h], rope_raw[d + 1, h]], axis=0).T for d in range(0, GROUP, 2)], axis=1)
        return carry

    lax.fori_loop(0, heads, turn_rope, 0)

    def place_rope(i, carry):
        rope_all[pl.ds(pl.multiple_of(i * heads, heads), heads)] = interleave(rope_turned, i)
        return carry

    lax.fori_loop(0, rows // heads, place_rope, 0)
    got_across(0).wait_recv()
    relay(0).start()
    lengths.wait()

    def chunk_step(g, carry):
        @pl.when(g + 1 < num_chunks)
        def _():
            got_across(g + 1).wait_recv()
            relay(g + 1).start()

        got_sibling(g).wait_recv()
        got_relay(g).wait_recv()

        def pair_step(p, lse_acc):
            step = g * per_chunk + p
            fetch(step).wait()

            @pl.when(step + SLOTS - 1 < steps)
            def _():
                fetch(step + SLOTS - 1).start()

            slot = step % SLOTS
            for i in range(PAIR):
                row = (first + step * PAIR + i) % rows
                q = jnp.concatenate([q_all[d, row] for d in range(GROUP)], axis=0)
                rope = rope_all[row]
                q_rope = jnp.concatenate([rope[:, d * ROPE_DIM:(d + 1) * ROPE_DIM] for d in range(GROUP)], axis=0)
                o, lse = attend(q, q_rope, ring[slot, i], me, len_ref[row])
                o_buf[step * PAIR + i] = o
                lane = lax.broadcasted_iota(jnp.int32, lse_acc.shape, 1)
                lse_acc = jnp.where(lane == p * PAIR + i, lse, lse_acc)
            return lse_acc

        lse_acc = lax.fori_loop(0, per_chunk, pair_step, jnp.zeros((GROUP * heads, 128), jnp.float32))
        columns = jnp.concatenate([lse_acc, lse_acc], axis=0).T
        half = CHUNK // 2
        left = lax.broadcasted_iota(jnp.int32, (half, 128), 1) < GROUP * heads
        lse_buf[g] = jnp.where(left, columns[:half], columns[half:CHUNK])

        @pl.when(g < 2 * quarter)
        def _():
            target = (1 - chip) * 2 + g // quarter
            for copy in send_part(g, 1 + (g // quarter + core) % 2, target):
                copy.start()

        @pl.when((g >= 2 * quarter) & (g // quarter - 2 != core))
        def _():
            for copy in send_part(g, 0, sibling):
                copy.start()

        return carry

    lax.fori_loop(0, num_chunks, chunk_step, 0)

    own_first = (2 + core) * quarter

    def drain(k, carry):
        send_across(k).wait_send()
        send_sibling(k).wait_send()
        relay(k).wait_send()
        return carry

    lax.fori_loop(0, num_chunks, drain, 0)
    send_rope(0, own_rope, me, across).wait_send()
    send_rope(1, own_rope, me, sibling).wait_send()
    send_rope(2, rope_raw.at[across], across, sibling).wait_send()

    def sent(k):
        for slot in range(GROUP - 1):
            for copy in send_part(k, slot, sibling):
                copy.wait_send()

    def merge_step(k, carry):
        @pl.when(k > 0)
        def _():
            sent(k - 1)

        arriving = [send_part(k, slot, sibling) for slot in range(GROUP - 1)]
        for copies in arriving:
            copies[-1].wait_recv()
        lses = [lse_buf[own_first + k]] + [lse_recv[slot, k] for slot in range(GROUP - 1)]
        top = functools.reduce(jnp.maximum, lses)
        total = top + jnp.log(functools.reduce(jnp.add, [jnp.exp(x - top) for x in lses]))
        factors = jnp.concatenate([jnp.exp(x - total) for x in lses], axis=0)
        padded = jnp.concatenate([factors, jnp.zeros((128 - factors.shape[0], 128), jnp.float32)], axis=0)
        columns = padded.T
        half = CHUNK // 2
        i = 0
        for piece, size in enumerate(PIECES):
            for copies in arriving:
                copies[piece].wait_recv()
            for i in range(i, i + size):
                factor = columns[i // half * GROUP * heads:(i // half + 1) * GROUP * heads]
                parts = [o_buf[(own_first + k) * CHUNK + i]] + [o_recv[slot, k, i] for slot in range(GROUP - 1)]
                merged = functools.reduce(jnp.add, [
                    factor[:, n * half + i % half:n * half + i % half + 1] * part.astype(jnp.float32)
                    for n, part in enumerate(parts)])
                out_ref[k * CHUNK + i] = merged.astype(jnp.bfloat16)
            i += 1
        return carry

    lax.fori_loop(0, quarter, merge_step, 0)
    sent(quarter - 1)


def solution(mesh):
    def local_step(q_blk, cache_blk, len_blk):
        rows, heads, width = q_blk.shape
        num_pages, page_len = cache_blk.shape[1], cache_blk.shape[3]
        cache_blk = jnp.swapaxes(cache_blk, 3, 4)
        latent = width - ROPE_DIM
        num_chunks = rows // CHUNK
        quarter = num_chunks // GROUP
        q_blk = jnp.transpose(q_blk, (1, 2, 0))
        dma = pltpu.SemaphoreType.DMA
        return pl.pallas_call(
            kernel,
            out_shape=pltpu.VMEM((rows // GROUP, GROUP * heads, latent), jnp.bfloat16),
            in_specs=[pl.BlockSpec(memory_space=pl.ANY), pl.BlockSpec(memory_space=pl.ANY),
                      pl.BlockSpec(memory_space=pl.ANY)],
            out_specs=pl.BlockSpec(memory_space=pltpu.VMEM),
            scratch_shapes=[
                pltpu.SMEM((rows,), jnp.int32),
                pltpu.VMEM((heads, latent, rows), jnp.bfloat16),
                pltpu.VMEM((heads, rows, latent), jnp.bfloat16),
                pltpu.VMEM((GROUP, rows, heads, latent), jnp.bfloat16),
                pltpu.VMEM((GROUP, heads, ROPE_DIM, rows), jnp.bfloat16),
                pltpu.VMEM((heads, rows, GROUP * ROPE_DIM), jnp.bfloat16),
                pltpu.VMEM((rows, heads, GROUP * ROPE_DIM), jnp.bfloat16),
                pltpu.VMEM((SLOTS, PAIR, num_pages, width, page_len), jnp.bfloat16),
                pltpu.VMEM((rows, GROUP * heads, latent), jnp.bfloat16),
                pltpu.VMEM((GROUP - 1, quarter, CHUNK, GROUP * heads, latent), jnp.bfloat16),
                pltpu.VMEM((num_chunks, CHUNK // 2, 128), jnp.float32),
                pltpu.VMEM((GROUP - 1, quarter, CHUNK // 2, 128), jnp.float32),
                dma(()), dma((2,)), dma((3,)), dma((3,)), dma((SLOTS,)),
                dma((num_chunks,)), dma((num_chunks,)), dma((num_chunks,)), dma((num_chunks,)),
                dma((num_chunks,)), dma((num_chunks,)),
                dma((GROUP - 1, quarter, len(PIECES))), dma((GROUP - 1, quarter, len(PIECES))),
                dma((GROUP - 1, quarter)), dma((GROUP - 1, quarter)),
                pltpu.SemaphoreType.REGULAR,
            ],
            compiler_params=pltpu.CompilerParams(collective_id=0, has_side_effects=True, vmem_limit_bytes=60 * 2**20),
        )(q_blk, cache_blk, len_blk)

    return jax.shard_map(local_step, mesh=mesh, in_specs=(P('dp', 'dcp', None), P('dp', None, 'dcp', None, None), P('dp')), out_specs=P(('dp', 'dcp'), None, None), check_vma=False)
```

```python
import functools
import math

import jax
import jax.numpy as jnp
from jax import lax
from jax.experimental import pallas as pl
from jax.experimental.pallas import tpu as pltpu
from jax.sharding import PartitionSpec as P

ROPE_DIM = 64
QK_DIM = 192
GROUP = 4
CHUNK = 16
PIECES = (12, 4)
PAIR = 2
SLOTS = 3


def attend(q, q_rope, cache, base, length):
    num_pages, width, page_len = cache.shape
    latent = width - ROPE_DIM
    scores = []
    for j in range(num_pages):
        page = (jnp.dot(q, cache[j, :latent], preferred_element_type=jnp.float32)
                + jnp.dot(q_rope, cache[j, latent:], preferred_element_type=jnp.float32))
        if j >= num_pages // 2:
            lane = lax.broadcasted_iota(jnp.int32, (1, page_len), 1)
            page = jnp.where(lane < length - (j * GROUP + base) * page_len, page, -jnp.inf)
        scores.append(page)
    top = jnp.max(functools.reduce(jnp.maximum, scores), axis=1, keepdims=True)
    scale = QK_DIM**-0.5
    weights = [jnp.exp2((page - top) * (scale * math.log2(math.e))) for page in scores]
    total = jnp.sum(functools.reduce(jnp.add, weights), axis=1, keepdims=True)
    mixed = functools.reduce(jnp.add, [
        lax.dot_general(weights[j].astype(jnp.bfloat16), cache[j, :latent], (((1,), (1,)), ((), ())),
                        preferred_element_type=jnp.float32) for j in range(num_pages)])
    return (mixed / total).astype(jnp.bfloat16), top * scale + jnp.log(total)


def kernel(q_hbm, cache_hbm, len_hbm, out_ref, len_ref, q_raw, q_turned, q_all, rope_raw, rope_turned, rope_all, ring, o_buf, o_recv, lse_buf, lse_recv, factor_buf,
           len_sem, own_sem, ps_sem, pr_sem, ring_sem, xs_sem, xr_sem, ds_sem, dr_sem, rs_sem, rr_sem, os_sem, or_sem, ls_sem, lr_sem, ready):
    heads, width, rows = q_hbm.shape
    latent = width - ROPE_DIM
    num_chunks = rows // CHUNK
    quarter = num_chunks // GROUP
    steps = rows // PAIR
    per_chunk = CHUNK // PAIR
    me = lax.axis_index("dcp")
    chip = me // 2
    core = me % 2
    across = (me + 2) % GROUP
    sibling = chip * 2 + (1 - core)
    diagonal = (sibling + 2) % GROUP
    first = (1 - chip) * (rows // 2)

    def start_row(k):
        return pl.multiple_of((first + k * CHUNK) % rows, CHUNK)

    def fetch(step):
        row = (first + step * PAIR) % rows
        slot = step % SLOTS
        return pltpu.make_async_copy(cache_hbm.at[pl.ds(row, PAIR), :, 0], ring.at[slot], ring_sem.at[slot])

    def send(src, dst, ssem, rsem, device):
        return pltpu.make_async_remote_copy(src_ref=src, dst_ref=dst, send_sem=ssem, recv_sem=rsem,
                                            device_id={"dcp": device}, device_id_type=pl.DeviceIdType.MESH)

    def send_across(k):
        row = pl.ds(pl.multiple_of((chip * (rows // 2) + k * CHUNK) % rows, CHUNK), CHUNK)
        return send(q_all.at[me, row], q_all.at[me, row], xs_sem.at[k], xr_sem.at[k], across)

    def got_across(k):
        row = pl.ds(start_row(k), CHUNK)
        return send(q_all.at[me, row], q_all.at[across, row], xs_sem.at[k], xr_sem.at[k], across)

    def send_sibling(k):
        row = pl.ds(start_row(k), CHUNK)
        return send(q_all.at[me, row], q_all.at[me, row], ds_sem.at[k], dr_sem.at[k], sibling)

    def got_sibling(k):
        row = pl.ds(start_row(k), CHUNK)
        return send(q_all.at[me, row], q_all.at[sibling, row], ds_sem.at[k], dr_sem.at[k], sibling)

    def relay(k):
        row = pl.ds(start_row(k), CHUNK)
        return send(q_all.at[across, row], q_all.at[across, row], rs_sem.at[k], rr_sem.at[k], sibling)

    def got_relay(k):
        row = pl.ds(start_row(k), CHUNK)
        return send(q_all.at[across, row], q_all.at[diagonal, row], rs_sem.at[k], rr_sem.at[k], sibling)

    def pieces(last):
        return PIECES if last else (CHUNK,)

    def send_part(g, slot, device, last):
        k = g % quarter
        copies, begin = [], 0
        for i, size in enumerate(pieces(last)):
            unit = math.gcd(begin, CHUNK)
            src = o_buf.at[pl.ds(pl.multiple_of(g * CHUNK + begin, unit), size)]
            copies.append(send(src, o_recv.at[slot, k, pl.ds(begin, size)],
                               os_sem.at[slot, k, i], or_sem.at[slot, k, i], device))
            begin += size
        lse = send(lse_buf.at[g], lse_recv.at[slot, k], ls_sem.at[slot, k], lr_sem.at[slot, k], device)
        return copies[:1] + [lse] + copies[1:]

    def start_part(g, slot, device):
        for last in (False, True):
            @pl.when((g % quarter == quarter - 1) == last)
            def _():
                for copy in send_part(g, slot, device, last):
                    copy.start()

    def send_rope(i, src, dst, device):
        return send(src, rope_raw.at[dst], ps_sem.at[i], pr_sem.at[i], device)

    def tell(semaphore, device):
        pl.semaphore_signal(semaphore, inc=1, device_id={"dcp": device}, device_id_type=pl.DeviceIdType.MESH)

    barrier = pltpu.get_barrier_semaphore()
    tell(barrier, across)

    own_rope = q_hbm.at[:, pl.ds(latent, ROPE_DIM), :]
    own = [pltpu.make_async_copy(q_hbm.at[:, pl.ds(0, latent), :], q_raw, own_sem.at[0]),
           pltpu.make_async_copy(own_rope, rope_raw.at[me], own_sem.at[1])]
    lengths = pltpu.make_async_copy(len_hbm, len_ref, len_sem)
    for copy in own + [lengths]:
        copy.start()
    for step in range(SLOTS - 1):
        fetch(step).start()

    pl.semaphore_wait(barrier, 3 - 2 * core)

    @pl.when(core == 1)
    def _():
        tell(barrier, sibling)
        tell(barrier, diagonal)

    @pl.when(core == 0)
    def _():
        tell(ready, sibling)
        tell(ready, diagonal)

    send_rope(0, own_rope, me, across).start()

    block = heads * heads
    into = lax.broadcasted_iota(jnp.int32, (block, block), 0)
    out_of = lax.broadcasted_iota(jnp.int32, (block, block), 1)
    swap = jnp.where(out_of == (into % heads) * heads + into // heads, 1.0, 0.0).astype(jnp.bfloat16)

    def interleave(turned, i):
        part = turned[:, pl.ds(pl.multiple_of(i * heads, heads), heads), :]
        lanes = part.shape[2]
        mixed = jnp.dot(swap, part.reshape(block, lanes), preferred_element_type=jnp.float32)
        return mixed.astype(jnp.bfloat16).reshape(heads, heads, lanes)

    own[0].wait()

    def turn(h, carry):
        q_turned[h] = q_raw[h].T
        return carry

    lax.fori_loop(0, heads, turn, 0)

    def place(i, carry):
        q_all[me, pl.ds(pl.multiple_of(i * heads, heads), heads)] = interleave(q_turned, i)
        return carry

    lax.fori_loop(0, rows // heads, place, 0)

    def issue_across(k, carry):
        send_across(k).start()
        return carry

    lax.fori_loop(0, num_chunks, issue_across, 0)

    @pl.when(core == 1)
    def _():
        pl.semaphore_wait(ready, 2)

    send_rope(1, own_rope, me, sibling).start()

    def issue_sibling(k, carry):
        send_sibling(k).start()
        return carry

    lax.fori_loop(0, num_chunks, issue_sibling, 0)
    send_rope(0, own_rope, across, across).wait_recv()
    send_rope(2, rope_raw.at[across], across, sibling).start()
    own[1].wait()
    send_rope(1, own_rope, sibling, sibling).wait_recv()
    send_rope(2, rope_raw.at[across], diagonal, sibling).wait_recv()

    def turn_rope(h, carry):
        rope_turned[h] = jnp.concatenate(
            [jnp.concatenate([rope_raw[d, h], rope_raw[d + 1, h]], axis=0).T for d in range(0, GROUP, 2)], axis=1)
        return carry

    lax.fori_loop(0, heads, turn_rope, 0)

    def place_rope(i, carry):
        rope_all[pl.ds(pl.multiple_of(i * heads, heads), heads)] = interleave(rope_turned, i)
        return carry

    lax.fori_loop(0, rows // heads, place_rope, 0)
    got_across(0).wait_recv()
    relay(0).start()
    lengths.wait()

    def chunk_step(g, carry):
        @pl.when(g + 1 < num_chunks)
        def _():
            got_across(g + 1).wait_recv()
            relay(g + 1).start()

        got_sibling(g).wait_recv()
        got_relay(g).wait_recv()

        def pair_step(p, lse_acc):
            step = g * per_chunk + p
            fetch(step).wait()

            @pl.when(step + SLOTS - 1 < steps)
            def _():
                fetch(step + SLOTS - 1).start()

            slot = step % SLOTS
            for i in range(PAIR):
                row = (first + step * PAIR + i) % rows
                q = jnp.concatenate([q_all[d, row] for d in range(GROUP)], axis=0)
                rope = rope_all[row]
                q_rope = jnp.concatenate([rope[:, d * ROPE_DIM:(d + 1) * ROPE_DIM] for d in range(GROUP)], axis=0)
                o, lse = attend(q, q_rope, ring[slot, i], me, len_ref[row])
                o_buf[step * PAIR + i] = o
                lane = lax.broadcasted_iota(jnp.int32, lse_acc.shape, 1)
                lse_acc = jnp.where(lane == p * PAIR + i, lse, lse_acc)
            return lse_acc

        lse_acc = lax.fori_loop(0, per_chunk, pair_step, jnp.zeros((GROUP * heads, 128), jnp.float32))
        columns = jnp.concatenate([lse_acc, lse_acc], axis=0).T
        half = CHUNK // 2
        left = lax.broadcasted_iota(jnp.int32, (half, 128), 1) < GROUP * heads
        lse_buf[g] = jnp.where(left, columns[:half], columns[half:CHUNK])

        @pl.when(g < 2 * quarter)
        def _():
            target = (1 - chip) * 2 + g // quarter
            start_part(g, 1 + (g // quarter + core) % 2, target)

        @pl.when((g >= 2 * quarter) & (g // quarter - 2 != core))
        def _():
            start_part(g, 0, sibling)

        return carry

    lax.fori_loop(0, num_chunks, chunk_step, 0)

    own_first = (2 + core) * quarter

    def drain(k, carry):
        send_across(k).wait_send()
        send_sibling(k).wait_send()
        relay(k).wait_send()
        return carry

    lax.fori_loop(0, num_chunks, drain, 0)
    send_rope(0, own_rope, me, across).wait_send()
    send_rope(1, own_rope, me, sibling).wait_send()
    send_rope(2, rope_raw.at[across], across, sibling).wait_send()

    def sent(k):
        for slot in range(GROUP - 1):
            for copy in send_part(k, slot, sibling, k == quarter - 1):
                copy.wait_send()

    step = PIECES[-1]
    half = CHUNK // 2
    every = GROUP * heads

    def wait_for(k, last, which):
        for slot in range(GROUP - 1):
            send_part(k, slot, sibling, last)[which].wait_recv()

    def merge_chunk(k, carry):
        last = k == quarter - 1
        wait_for(k, False, 1)
        lses = [lse_buf[own_first + k]] + [lse_recv[slot, k] for slot in range(GROUP - 1)]
        top = functools.reduce(jnp.maximum, lses)
        total = top + jnp.log(functools.reduce(jnp.add, [jnp.exp(x - top) for x in lses]))
        factors = jnp.concatenate([jnp.exp(x - total) for x in lses], axis=0)
        padded = jnp.concatenate([factors, jnp.zeros((128 - factors.shape[0], 128), jnp.float32)], axis=0)
        factor_buf[...] = padded.T
        for final in (False, True):
            @pl.when(last == final)
            def _():
                wait_for(k, final, 0)

        def merge_piece(m, carry):
            @pl.when(last & (m == CHUNK // step - 1))
            def _():
                wait_for(k, True, 2)

            factor = factor_buf[pl.ds(pl.multiple_of(m * step // half * every, every), every)]
            factor = jnp.where(m * step % half > 0, pltpu.roll(factor, 128 - step, 1), factor)
            for i in range(step):
                row = m * step + i
                parts = [o_buf[(own_first + k) * CHUNK + row]] + [o_recv[slot, k, row] for slot in range(GROUP - 1)]
                merged = functools.reduce(jnp.add, [
                    factor[:, n * half + i:n * half + i + 1] * part.astype(jnp.float32) for n, part in enumerate(parts)])
                out_ref[k * CHUNK + row] = merged.astype(jnp.bfloat16)
            return carry

        return lax.fori_loop(0, CHUNK // step, merge_piece, carry)

    lax.fori_loop(0, quarter, merge_chunk, 0)
    for k in range(quarter):
        sent(k)


def solution(mesh):
    def local_step(q_blk, cache_blk, len_blk):
        rows, heads, width = q_blk.shape
        num_pages, page_len = cache_blk.shape[1], cache_blk.shape[3]
        cache_blk = jnp.swapaxes(cache_blk, 3, 4)
        latent = width - ROPE_DIM
        num_chunks = rows // CHUNK
        quarter = num_chunks // GROUP
        q_blk = jnp.transpose(q_blk, (1, 2, 0))
        dma = pltpu.SemaphoreType.DMA
        return pl.pallas_call(
            kernel,
            out_shape=pltpu.VMEM((rows // GROUP, GROUP * heads, latent), jnp.bfloat16),
            in_specs=[pl.BlockSpec(memory_space=pl.ANY), pl.BlockSpec(memory_space=pl.ANY),
                      pl.BlockSpec(memory_space=pl.ANY)],
            out_specs=pl.BlockSpec(memory_space=pltpu.VMEM),
            scratch_shapes=[
                pltpu.SMEM((rows,), jnp.int32),
                pltpu.VMEM((heads, latent, rows), jnp.bfloat16),
                pltpu.VMEM((heads, rows, latent), jnp.bfloat16),
                pltpu.VMEM((GROUP, rows, heads, latent), jnp.bfloat16),
                pltpu.VMEM((GROUP, heads, ROPE_DIM, rows), jnp.bfloat16),
                pltpu.VMEM((heads, rows, GROUP * ROPE_DIM), jnp.bfloat16),
                pltpu.VMEM((rows, heads, GROUP * ROPE_DIM), jnp.bfloat16),
                pltpu.VMEM((SLOTS, PAIR, num_pages, width, page_len), jnp.bfloat16),
                pltpu.VMEM((rows, GROUP * heads, latent), jnp.bfloat16),
                pltpu.VMEM((GROUP - 1, quarter, CHUNK, GROUP * heads, latent), jnp.bfloat16),
                pltpu.VMEM((num_chunks, CHUNK // 2, 128), jnp.float32),
                pltpu.VMEM((GROUP - 1, quarter, CHUNK // 2, 128), jnp.float32),
                pltpu.VMEM((128, 128), jnp.float32),
                dma(()), dma((2,)), dma((3,)), dma((3,)), dma((SLOTS,)),
                dma((num_chunks,)), dma((num_chunks,)), dma((num_chunks,)), dma((num_chunks,)),
                dma((num_chunks,)), dma((num_chunks,)),
                dma((GROUP - 1, quarter, len(PIECES))), dma((GROUP - 1, quarter, len(PIECES))),
                dma((GROUP - 1, quarter)), dma((GROUP - 1, quarter)),
                pltpu.SemaphoreType.REGULAR,
            ],
            compiler_params=pltpu.CompilerParams(collective_id=0, has_side_effects=True, vmem_limit_bytes=60 * 2**20),
        )(q_blk, cache_blk, len_blk)

    return jax.shard_map(local_step, mesh=mesh, in_specs=(P('dp', 'dcp', None), P('dp', None, 'dcp', None, None), P('dp')), out_specs=P(('dp', 'dcp'), None, None), check_vma=False)
```

```python
import functools
import math

import jax
import jax.numpy as jnp
from jax import lax
from jax.experimental import pallas as pl
from jax.experimental.pallas import tpu as pltpu
from jax.sharding import PartitionSpec as P

ROPE_DIM = 64
QK_DIM = 192
GROUP = 4
CHUNK = 16
PIECES = (12, 4)
PAIR = 2
SLOTS = 3


def attend(q, q_rope, cache, base, length):
    num_pages, width, page_len = cache.shape
    latent = width - ROPE_DIM
    scores = []
    for j in range(num_pages):
        page = (jnp.dot(q, cache[j, :latent], preferred_element_type=jnp.float32)
                + jnp.dot(q_rope, cache[j, latent:], preferred_element_type=jnp.float32))
        if j >= num_pages // 2:
            lane = lax.broadcasted_iota(jnp.int32, (1, page_len), 1)
            page = jnp.where(lane < length - (j * GROUP + base) * page_len, page, -jnp.inf)
        scores.append(page)
    top = jnp.max(functools.reduce(jnp.maximum, scores), axis=1, keepdims=True)
    scale = QK_DIM**-0.5
    weights = [jnp.exp2((page - top) * (scale * math.log2(math.e))) for page in scores]
    total = jnp.sum(functools.reduce(jnp.add, weights), axis=1, keepdims=True)
    mixed = functools.reduce(jnp.add, [
        lax.dot_general(weights[j].astype(jnp.bfloat16), cache[j, :latent], (((1,), (1,)), ((), ())),
                        preferred_element_type=jnp.float32) for j in range(num_pages)])
    return (mixed / total).astype(jnp.bfloat16), top * scale + jnp.log(total)


def kernel(q_hbm, cache_hbm, len_hbm, out_ref, len_ref, q_raw, q_turned, q_all, rope_raw, rope_turned, rope_all, ring, o_buf, o_recv, lse_buf, lse_recv, factor_buf,
           len_sem, own_sem, ps_sem, pr_sem, ring_sem, qs_sem, xr_sem, dr_sem, rr_sem, os_sem, or_sem, ls_sem, lr_sem, ready):
    heads, width, rows = q_hbm.shape
    latent = width - ROPE_DIM
    num_chunks = rows // CHUNK
    quarter = num_chunks // GROUP
    steps = rows // PAIR
    per_chunk = CHUNK // PAIR
    me = lax.axis_index("dcp")
    chip = me // 2
    core = me % 2
    across = (me + 2) % GROUP
    sibling = chip * 2 + (1 - core)
    diagonal = (sibling + 2) % GROUP
    first = (1 - chip) * (rows // 2)

    def start_row(k):
        return pl.multiple_of((first + k * CHUNK) % rows, CHUNK)

    def fetch(step):
        row = (first + step * PAIR) % rows
        slot = step % SLOTS
        return pltpu.make_async_copy(cache_hbm.at[pl.ds(row, PAIR), :, 0], ring.at[slot], ring_sem.at[slot])

    def send(src, dst, ssem, rsem, device):
        return pltpu.make_async_remote_copy(src_ref=src, dst_ref=dst, send_sem=ssem, recv_sem=rsem,
                                            device_id={"dcp": device}, device_id_type=pl.DeviceIdType.MESH)

    groups = [(0, 1)] + [(2**i, 2**i) for i in range(num_chunks.bit_length() - 1)]

    def rows_of(i, begin_at):
        start, size = groups[i]
        return pl.ds(pl.multiple_of((begin_at + start * CHUNK) % rows, CHUNK), size * CHUNK)

    def send_across(i):
        row = rows_of(i, chip * (rows // 2))
        return send(q_all.at[me, row], q_all.at[me, row], qs_sem, xr_sem.at[i], across)

    def got_across(i):
        row = rows_of(i, first)
        return send(q_all.at[me, row], q_all.at[across, row], qs_sem, xr_sem.at[i], across)

    def send_sibling():
        return send(q_all.at[me], q_all.at[me], qs_sem, dr_sem, sibling)

    def got_sibling():
        return send(q_all.at[me], q_all.at[sibling], qs_sem, dr_sem, sibling)

    def relay(i):
        row = rows_of(i, first)
        return send(q_all.at[across, row], q_all.at[across, row], qs_sem, rr_sem.at[i], sibling)

    def got_relay(i):
        row = rows_of(i, first)
        return send(q_all.at[across, row], q_all.at[diagonal, row], qs_sem, rr_sem.at[i], sibling)

    def wait_bytes(ref, semaphore):
        pltpu.make_async_copy(ref, ref, semaphore).wait()

    def pieces(last):
        return PIECES if last else (CHUNK,)

    def send_part(g, slot, device, last):
        k = g % quarter
        copies, begin = [], 0
        for i, size in enumerate(pieces(last)):
            unit = math.gcd(begin, CHUNK)
            src = o_buf.at[pl.ds(pl.multiple_of(g * CHUNK + begin, unit), size)]
            copies.append(send(src, o_recv.at[slot, k, pl.ds(begin, size)], os_sem, or_sem.at[k + i], device))
            begin += size
        lse = send(lse_buf.at[g], lse_recv.at[slot, k], ls_sem, lr_sem.at[k], device)
        return copies[:1] + [lse] + copies[1:]

    def start_part(g, slot, device):
        for last in (False, True):
            @pl.when((g % quarter == quarter - 1) == last)
            def _():
                for copy in send_part(g, slot, device, last):
                    copy.start()

    def send_rope(i, src, dst, device):
        return send(src, rope_raw.at[dst], ps_sem, pr_sem.at[i], device)

    def tell(semaphore, device):
        pl.semaphore_signal(semaphore, inc=1, device_id={"dcp": device}, device_id_type=pl.DeviceIdType.MESH)

    barrier = pltpu.get_barrier_semaphore()
    tell(barrier, across)

    own_rope = q_hbm.at[:, pl.ds(latent, ROPE_DIM), :]
    own = [pltpu.make_async_copy(q_hbm.at[:, pl.ds(0, latent), :], q_raw, own_sem.at[0]),
           pltpu.make_async_copy(own_rope, rope_raw.at[me], own_sem.at[1])]
    lengths = pltpu.make_async_copy(len_hbm, len_ref, len_sem)
    for copy in own + [lengths]:
        copy.start()
    for step in range(SLOTS - 1):
        fetch(step).start()

    pl.semaphore_wait(barrier, 3 - 2 * core)

    @pl.when(core == 1)
    def _():
        tell(barrier, sibling)
        tell(barrier, diagonal)

    @pl.when(core == 0)
    def _():
        tell(ready, sibling)
        tell(ready, diagonal)

    send_rope(0, own_rope, me, across).start()

    block = heads * heads
    into = lax.broadcasted_iota(jnp.int32, (block, block), 0)
    out_of = lax.broadcasted_iota(jnp.int32, (block, block), 1)
    swap = jnp.where(out_of == (into % heads) * heads + into // heads, 1.0, 0.0).astype(jnp.bfloat16)

    def interleave(turned, i):
        part = turned[:, pl.ds(pl.multiple_of(i * heads, heads), heads), :]
        lanes = part.shape[2]
        mixed = jnp.dot(swap, part.reshape(block, lanes), preferred_element_type=jnp.float32)
        return mixed.astype(jnp.bfloat16).reshape(heads, heads, lanes)

    own[0].wait()

    def turn(h, carry):
        q_turned[h] = q_raw[h].T
        return carry

    lax.fori_loop(0, heads, turn, 0)

    def place(i, carry):
        q_all[me, pl.ds(pl.multiple_of(i * heads, heads), heads)] = interleave(q_turned, i)
        return carry

    lax.fori_loop(0, rows // heads, place, 0)

    for i in range(len(groups)):
        send_across(i).start()

    @pl.when(core == 1)
    def _():
        pl.semaphore_wait(ready, 2)

    send_rope(1, own_rope, me, sibling).start()

    send_sibling().start()
    send_rope(0, own_rope, across, across).wait_recv()
    send_rope(2, rope_raw.at[across], across, sibling).start()
    own[1].wait()
    send_rope(1, own_rope, sibling, sibling).wait_recv()
    send_rope(2, rope_raw.at[across], diagonal, sibling).wait_recv()

    def turn_rope(h, carry):
        rope_turned[h] = jnp.concatenate(
            [jnp.concatenate([rope_raw[d, h], rope_raw[d + 1, h]], axis=0).T for d in range(0, GROUP, 2)], axis=1)
        return carry

    lax.fori_loop(0, heads, turn_rope, 0)

    def place_rope(i, carry):
        rope_all[pl.ds(pl.multiple_of(i * heads, heads), heads)] = interleave(rope_turned, i)
        return carry

    lax.fori_loop(0, rows // heads, place_rope, 0)
    got_across(0).wait_recv()
    relay(0).start()
    lengths.wait()
    got_sibling().wait_recv()

    def chunk_step(g, carry):
        for i, (start, _) in enumerate(groups):
            if i > 0:
                @pl.when(g + 1 == start)
                def _():
                    got_across(i).wait_recv()
                    relay(i).start()

            @pl.when(g == start)
            def _():
                got_relay(i).wait_recv()

        def pair_step(p, lse_acc):
            step = g * per_chunk + p
            fetch(step).wait()

            @pl.when(step + SLOTS - 1 < steps)
            def _():
                fetch(step + SLOTS - 1).start()

            slot = step % SLOTS
            for i in range(PAIR):
                row = (first + step * PAIR + i) % rows
                q = jnp.concatenate([q_all[d, row] for d in range(GROUP)], axis=0)
                rope = rope_all[row]
                q_rope = jnp.concatenate([rope[:, d * ROPE_DIM:(d + 1) * ROPE_DIM] for d in range(GROUP)], axis=0)
                o, lse = attend(q, q_rope, ring[slot, i], me, len_ref[row])
                o_buf[step * PAIR + i] = o
                lane = lax.broadcasted_iota(jnp.int32, lse_acc.shape, 1)
                lse_acc = jnp.where(lane == p * PAIR + i, lse, lse_acc)
            return lse_acc

        lse_acc = lax.fori_loop(0, per_chunk, pair_step, jnp.zeros((GROUP * heads, 128), jnp.float32))
        columns = jnp.concatenate([lse_acc, lse_acc], axis=0).T
        half = CHUNK // 2
        left = lax.broadcasted_iota(jnp.int32, (half, 128), 1) < GROUP * heads
        lse_buf[g] = jnp.where(left, columns[:half], columns[half:CHUNK])

        @pl.when(g < 2 * quarter)
        def _():
            target = (1 - chip) * 2 + g // quarter
            start_part(g, 1 + (g // quarter + core) % 2, target)

        @pl.when((g >= 2 * quarter) & (g // quarter - 2 != core))
        def _():
            start_part(g, 0, sibling)

        return carry

    lax.fori_loop(0, num_chunks, chunk_step, 0)

    own_first = (2 + core) * quarter

    wait_bytes(q_all.at[pl.ds(0, GROUP - 1)], qs_sem)
    wait_bytes(rope_raw.at[pl.ds(0, GROUP - 1)], ps_sem)

    step = PIECES[-1]
    half = CHUNK // 2
    every = GROUP * heads

    def wait_for(k, last, i):
        begin = sum(pieces(last)[:i])
        wait_bytes(o_recv.at[:, k, pl.ds(begin, pieces(last)[i])], or_sem.at[k + i])

    def merge_chunk(k, carry):
        last = k == quarter - 1
        wait_bytes(lse_recv.at[:, k], lr_sem.at[k])
        lses = [lse_buf[own_first + k]] + [lse_recv[slot, k] for slot in range(GROUP - 1)]
        top = functools.reduce(jnp.maximum, lses)
        total = top + jnp.log(functools.reduce(jnp.add, [jnp.exp(x - top) for x in lses]))
        factors = jnp.concatenate([jnp.exp(x - total) for x in lses], axis=0)
        padded = jnp.concatenate([factors, jnp.zeros((128 - factors.shape[0], 128), jnp.float32)], axis=0)
        factor_buf[...] = padded.T
        for final in (False, True):
            @pl.when(last == final)
            def _():
                wait_for(k, final, 0)

        def merge_piece(m, carry):
            @pl.when(last & (m == CHUNK // step - 1))
            def _():
                wait_for(k, True, 1)

            factor = factor_buf[pl.ds(pl.multiple_of(m * step // half * every, every), every)]
            factor = jnp.where(m * step % half > 0, pltpu.roll(factor, 128 - step, 1), factor)
            for i in range(step):
                row = m * step + i
                parts = [o_buf[(own_first + k) * CHUNK + row]] + [o_recv[slot, k, row] for slot in range(GROUP - 1)]
                merged = functools.reduce(jnp.add, [
                    factor[:, n * half + i:n * half + i + 1] * part.astype(jnp.float32) for n, part in enumerate(parts)])
                out_ref[k * CHUNK + row] = merged.astype(jnp.bfloat16)
            return carry

        return lax.fori_loop(0, CHUNK // step, merge_piece, carry)

    lax.fori_loop(0, quarter, merge_chunk, 0)
    wait_bytes(o_buf.at[pl.ds(0, (GROUP - 1) * quarter * CHUNK)], os_sem)
    wait_bytes(lse_buf.at[pl.ds(0, (GROUP - 1) * quarter)], ls_sem)


def solution(mesh):
    def local_step(q_blk, cache_blk, len_blk):
        rows, heads, width = q_blk.shape
        num_pages, page_len = cache_blk.shape[1], cache_blk.shape[3]
        cache_blk = jnp.swapaxes(cache_blk, 3, 4)
        latent = width - ROPE_DIM
        num_chunks = rows // CHUNK
        quarter = num_chunks // GROUP
        q_blk = jnp.transpose(q_blk, (1, 2, 0))
        dma = pltpu.SemaphoreType.DMA
        return pl.pallas_call(
            kernel,
            out_shape=pltpu.VMEM((rows // GROUP, GROUP * heads, latent), jnp.bfloat16),
            in_specs=[pl.BlockSpec(memory_space=pl.ANY), pl.BlockSpec(memory_space=pl.ANY),
                      pl.BlockSpec(memory_space=pl.ANY)],
            out_specs=pl.BlockSpec(memory_space=pltpu.VMEM),
            scratch_shapes=[
                pltpu.SMEM((rows,), jnp.int32),
                pltpu.VMEM((heads, latent, rows), jnp.bfloat16),
                pltpu.VMEM((heads, rows, latent), jnp.bfloat16),
                pltpu.VMEM((GROUP, rows, heads, latent), jnp.bfloat16),
                pltpu.VMEM((GROUP, heads, ROPE_DIM, rows), jnp.bfloat16),
                pltpu.VMEM((heads, rows, GROUP * ROPE_DIM), jnp.bfloat16),
                pltpu.VMEM((rows, heads, GROUP * ROPE_DIM), jnp.bfloat16),
                pltpu.VMEM((SLOTS, PAIR, num_pages, width, page_len), jnp.bfloat16),
                pltpu.VMEM((rows, GROUP * heads, latent), jnp.bfloat16),
                pltpu.VMEM((GROUP - 1, quarter, CHUNK, GROUP * heads, latent), jnp.bfloat16),
                pltpu.VMEM((num_chunks, CHUNK // 2, 128), jnp.float32),
                pltpu.VMEM((GROUP - 1, quarter, CHUNK // 2, 128), jnp.float32),
                pltpu.VMEM((128, 128), jnp.float32),
                dma(()), dma((2,)), dma(()), dma((3,)), dma((SLOTS,)),
                dma(()), dma((num_chunks.bit_length(),)), dma(()), dma((num_chunks.bit_length(),)),
                dma(()), dma((quarter + len(PIECES) - 1,)), dma(()), dma((quarter,)),
                pltpu.SemaphoreType.REGULAR,
            ],
            compiler_params=pltpu.CompilerParams(collective_id=0, has_side_effects=True, vmem_limit_bytes=60 * 2**20),
        )(q_blk, cache_blk, len_blk)

    return jax.shard_map(local_step, mesh=mesh, in_specs=(P('dp', 'dcp', None), P('dp', None, 'dcp', None, None), P('dp')), out_specs=P(('dp', 'dcp'), None, None), check_vma=False)
```

```python
import functools
import math

import jax
import jax.numpy as jnp
from jax import lax
from jax.experimental import pallas as pl
from jax.experimental.pallas import tpu as pltpu
from jax.sharding import PartitionSpec as P

ROPE_DIM = 64
QK_DIM = 192
GROUP = 4
CHUNK = 16
PIECES = (12, 4)
PAIR = 2
SIBLING = 0
SLOTS = 3


def attend(q, q_rope, cache, base, length):
    num_pages, width, page_len = cache.shape
    latent = width - ROPE_DIM
    scores = []
    for j in range(num_pages):
        page = (jnp.dot(q, cache[j, :latent], preferred_element_type=jnp.float32)
                + jnp.dot(q_rope, cache[j, latent:], preferred_element_type=jnp.float32))
        if j >= num_pages // 2:
            lane = lax.broadcasted_iota(jnp.int32, (1, page_len), 1)
            page = jnp.where(lane < length - (j * GROUP + base) * page_len, page, -jnp.inf)
        scores.append(page)
    top = jnp.max(functools.reduce(jnp.maximum, scores), axis=1, keepdims=True)
    scale = QK_DIM**-0.5
    weights = [jnp.exp2((page - top) * (scale * math.log2(math.e))) for page in scores]
    total = jnp.sum(functools.reduce(jnp.add, weights), axis=1, keepdims=True)
    mixed = functools.reduce(jnp.add, [
        lax.dot_general(weights[j].astype(jnp.bfloat16), cache[j, :latent], (((1,), (1,)), ((), ())),
                        preferred_element_type=jnp.float32) for j in range(num_pages)])
    return (mixed / total).astype(jnp.bfloat16), top * scale + jnp.log(total)


def mix(factor, parts, i, first=0):
    half = CHUNK // 2
    return functools.reduce(jnp.add, [
        factor[:, n * half + i:n * half + i + 1] * part.astype(jnp.float32) for n, part in enumerate(parts, first)])


def store(early, tail, base, factor, out_hbm, buf, sems):
    done = early.shape[0]
    copies = [pltpu.make_async_copy(early, out_hbm.at[pl.ds(0, done)], sems.at[0]),
              pltpu.make_async_copy(buf, out_hbm.at[pl.ds(done, buf.shape[0])], sems.at[1])]
    copies[0].start()
    for i in range(buf.shape[0]):
        merged = base[i] + mix(factor[...], [tail[0, i]], i, 2) + mix(factor[...], [tail[1, i]], i, 3)
        buf[i] = merged.astype(jnp.bfloat16)
    copies[1].start()
    for copy in copies:
        copy.wait()


def kernel(q_hbm, cache_hbm, len_hbm, out_ref, tail_ref, base_ref, tail_factor, len_ref, q_raw, q_turned, q_all, rope_raw, rope_turned, rope_all, ring, o_buf, o_recv, lse_buf, lse_recv, factor_buf, stage,
           len_sem, own_sem, ps_sem, pr_sem, ring_sem, qs_sem, xr_sem, dr_sem, rr_sem, os_sem, or_sem, ls_sem, lr_sem, hs_sem, hr_sem, ready):
    heads, width, rows = q_hbm.shape
    latent = width - ROPE_DIM
    num_chunks = rows // CHUNK
    quarter = num_chunks // GROUP
    steps = rows // PAIR
    per_chunk = CHUNK // PAIR
    me = lax.axis_index("dcp")
    chip = me // 2
    core = me % 2
    across = (me + 2) % GROUP
    sibling = chip * 2 + (1 - core)
    diagonal = (sibling + 2) % GROUP
    first = (1 - chip) * (rows // 2)

    def start_row(k):
        return pl.multiple_of((first + k * CHUNK) % rows, CHUNK)

    def fetch(step):
        row = (first + step * PAIR) % rows
        slot = step % SLOTS
        return pltpu.make_async_copy(cache_hbm.at[pl.ds(row, PAIR), :, 0], ring.at[slot], ring_sem.at[slot])

    def send(src, dst, ssem, rsem, device):
        return pltpu.make_async_remote_copy(src_ref=src, dst_ref=dst, send_sem=ssem, recv_sem=rsem,
                                            device_id={"dcp": device}, device_id_type=pl.DeviceIdType.MESH)

    groups = [(0, 1)] + [(2**i, 2**i) for i in range(num_chunks.bit_length() - 1)]

    def rows_of(i, begin_at):
        start, size = groups[i]
        return pl.ds(pl.multiple_of((begin_at + start * CHUNK) % rows, CHUNK), size * CHUNK)

    def send_across(i):
        row = rows_of(i, chip * (rows // 2))
        return send(q_all.at[me, row], q_all.at[me, row], qs_sem, xr_sem.at[i], across)

    def got_across(i):
        row = rows_of(i, first)
        return send(q_all.at[me, row], q_all.at[across, row], qs_sem, xr_sem.at[i], across)

    def send_sibling():
        return send(q_all.at[me], q_all.at[me], qs_sem, dr_sem, sibling)

    def got_sibling():
        return send(q_all.at[me], q_all.at[sibling], qs_sem, dr_sem, sibling)

    def relay(i):
        row = rows_of(i, first)
        return send(q_all.at[across, row], q_all.at[across, row], qs_sem, rr_sem.at[i], sibling)

    def got_relay(i):
        row = rows_of(i, first)
        return send(q_all.at[across, row], q_all.at[diagonal, row], qs_sem, rr_sem.at[i], sibling)

    def wait_bytes(ref, semaphore):
        pltpu.make_async_copy(ref, ref, semaphore).wait()

    tail = PIECES[-1]
    kept = CHUNK - tail

    def send_part(g, slot, device, last):
        k = g % quarter
        split = last and slot is not SIBLING

        def part(begin, size, dst, semaphore):
            src = o_buf.at[pl.ds(pl.multiple_of(g * CHUNK + begin, math.gcd(begin, CHUNK)), size)]
            return send(src, dst, os_sem, semaphore, device)

        size = kept if split else CHUNK
        copies = [part(0, size, o_recv.at[slot, k, pl.ds(0, size)], or_sem.at[k]),
                  send(lse_buf.at[g], lse_recv.at[slot, k], ls_sem, lr_sem.at[k], device)]
        if split:
            copies.append(part(kept, tail, tail_ref.at[slot - 1], or_sem.at[quarter]))
        return copies

    crossing = 2 * quarter

    def hand_over():
        return send(o_buf.at[pl.ds(crossing * CHUNK - tail, tail)], stage, os_sem, hr_sem, sibling)

    def send_handed():
        return send(stage, tail_ref.at[1], hs_sem, or_sem.at[quarter], across)

    def start_part(g, slot, device):
        for last in (False, True):
            @pl.when((g % quarter == quarter - 1) == last)
            def _():
                copies = send_part(g, slot, device, last)
                for copy in copies[:2]:
                    copy.start()
                if len(copies) > 2:
                    handed = (g == crossing - 1) & (core == 0)

                    @pl.when(handed)
                    def _():
                        hand_over().start()

                    @pl.when(jnp.logical_not(handed))
                    def _():
                        copies[2].start()

    def send_rope(i, src, dst, device):
        return send(src, rope_raw.at[dst], ps_sem, pr_sem.at[i], device)

    def tell(semaphore, device):
        pl.semaphore_signal(semaphore, inc=1, device_id={"dcp": device}, device_id_type=pl.DeviceIdType.MESH)

    barrier = pltpu.get_barrier_semaphore()
    tell(barrier, across)

    own_rope = q_hbm.at[:, pl.ds(latent, ROPE_DIM), :]
    own = [pltpu.make_async_copy(q_hbm.at[:, pl.ds(0, latent), :], q_raw, own_sem.at[0]),
           pltpu.make_async_copy(own_rope, rope_raw.at[me], own_sem.at[1])]
    lengths = pltpu.make_async_copy(len_hbm, len_ref, len_sem)
    for copy in own + [lengths]:
        copy.start()
    for step in range(SLOTS - 1):
        fetch(step).start()

    pl.semaphore_wait(barrier, 3 - 2 * core)

    @pl.when(core == 1)
    def _():
        tell(barrier, sibling)
        tell(barrier, diagonal)

    @pl.when(core == 0)
    def _():
        tell(ready, sibling)
        tell(ready, diagonal)

    send_rope(0, own_rope, me, across).start()

    block = heads * heads
    into = lax.broadcasted_iota(jnp.int32, (block, block), 0)
    out_of = lax.broadcasted_iota(jnp.int32, (block, block), 1)
    swap = jnp.where(out_of == (into % heads) * heads + into // heads, 1.0, 0.0).astype(jnp.bfloat16)

    def interleave(turned, i):
        part = turned[:, pl.ds(pl.multiple_of(i * heads, heads), heads), :]
        lanes = part.shape[2]
        mixed = jnp.dot(swap, part.reshape(block, lanes), preferred_element_type=jnp.float32)
        return mixed.astype(jnp.bfloat16).reshape(heads, heads, lanes)

    own[0].wait()

    def turn(h, carry):
        q_turned[h] = q_raw[h].T
        return carry

    lax.fori_loop(0, heads, turn, 0)

    def place(i, carry):
        q_all[me, pl.ds(pl.multiple_of(i * heads, heads), heads)] = interleave(q_turned, i)
        return carry

    lax.fori_loop(0, rows // heads, place, 0)

    for i in range(len(groups)):
        send_across(i).start()

    @pl.when(core == 1)
    def _():
        pl.semaphore_wait(ready, 2)

    send_rope(1, own_rope, me, sibling).start()

    send_sibling().start()
    send_rope(0, own_rope, across, across).wait_recv()
    send_rope(2, rope_raw.at[across], across, sibling).start()
    own[1].wait()
    send_rope(1, own_rope, sibling, sibling).wait_recv()
    send_rope(2, rope_raw.at[across], diagonal, sibling).wait_recv()

    def turn_rope(h, carry):
        rope_turned[h] = jnp.concatenate(
            [jnp.concatenate([rope_raw[d, h], rope_raw[d + 1, h]], axis=0).T for d in range(0, GROUP, 2)], axis=1)
        return carry

    lax.fori_loop(0, heads, turn_rope, 0)

    def place_rope(i, carry):
        rope_all[pl.ds(pl.multiple_of(i * heads, heads), heads)] = interleave(rope_turned, i)
        return carry

    lax.fori_loop(0, rows // heads, place_rope, 0)
    got_across(0).wait_recv()
    relay(0).start()
    lengths.wait()
    got_sibling().wait_recv()

    def chunk_step(g, carry):
        for i, (start, _) in enumerate(groups):
            if i > 0:
                @pl.when(g + 1 == start)
                def _():
                    got_across(i).wait_recv()
                    relay(i).start()

            @pl.when(g == start)
            def _():
                got_relay(i).wait_recv()

        @pl.when((g == crossing + 1) & (core == 1))
        def _():
            hand_over().wait_recv()
            send_handed().start()

        def pair_step(p, lse_acc):
            step = g * per_chunk + p
            fetch(step).wait()

            @pl.when(step + SLOTS - 1 < steps)
            def _():
                fetch(step + SLOTS - 1).start()

            slot = step % SLOTS
            for i in range(PAIR):
                row = (first + step * PAIR + i) % rows
                q = jnp.concatenate([q_all[d, row] for d in range(GROUP)], axis=0)
                rope = rope_all[row]
                q_rope = jnp.concatenate([rope[:, d * ROPE_DIM:(d + 1) * ROPE_DIM] for d in range(GROUP)], axis=0)
                o, lse = attend(q, q_rope, ring[slot, i], me, len_ref[row])
                o_buf[step * PAIR + i] = o
                lane = lax.broadcasted_iota(jnp.int32, lse_acc.shape, 1)
                lse_acc = jnp.where(lane == p * PAIR + i, lse, lse_acc)
            return lse_acc

        lse_acc = lax.fori_loop(0, per_chunk, pair_step, jnp.zeros((GROUP * heads, 128), jnp.float32))
        columns = jnp.concatenate([lse_acc, lse_acc], axis=0).T
        half = CHUNK // 2
        left = lax.broadcasted_iota(jnp.int32, (half, 128), 1) < GROUP * heads
        lse_buf[g] = jnp.where(left, columns[:half], columns[half:CHUNK])

        @pl.when(g < 2 * quarter)
        def _():
            target = (1 - chip) * 2 + g // quarter
            start_part(g, 1 + (g // quarter + core) % 2, target)

        @pl.when((g >= 2 * quarter) & (g // quarter - 2 != core))
        def _():
            start_part(g, SIBLING, sibling)

        return carry

    lax.fori_loop(0, num_chunks, chunk_step, 0)

    own_first = (2 + core) * quarter

    wait_bytes(q_all.at[pl.ds(0, GROUP - 1)], qs_sem)
    wait_bytes(rope_raw.at[pl.ds(0, GROUP - 1)], ps_sem)

    half = CHUNK // 2
    every = GROUP * heads

    def factors_of(k):
        wait_bytes(lse_recv.at[:, k], lr_sem.at[k])
        lses = [lse_buf[own_first + k]] + [lse_recv[slot, k] for slot in range(GROUP - 1)]
        top = functools.reduce(jnp.maximum, lses)
        total = top + jnp.log(functools.reduce(jnp.add, [jnp.exp(x - top) for x in lses]))
        factors = jnp.concatenate([jnp.exp(x - total) for x in lses], axis=0)
        padded = jnp.concatenate([factors, jnp.zeros((128 - factors.shape[0], 128), jnp.float32)], axis=0)
        factor_buf[...] = padded.T

    def factor_at(m):
        factor = factor_buf[pl.ds(pl.multiple_of(m * tail // half * every, every), every)]
        return jnp.where(m * tail % half > 0, pltpu.roll(factor, 128 - tail, 1), factor)

    def merge_chunk(k, carry):
        last = k == quarter - 1
        factors_of(k)

        @pl.when(jnp.logical_not(last))
        def _():
            wait_bytes(o_buf.at[pl.ds(0, (GROUP - 1) * CHUNK)], or_sem.at[k])

        @pl.when(last)
        def _():
            wait_bytes(o_buf.at[pl.ds(0, (GROUP - 1) * CHUNK - 2 * tail)], or_sem.at[k])

        def merge_piece(m, carry):
            factor = factor_at(m)
            for i in range(tail):
                row = m * tail + i
                parts = [o_buf[(own_first + k) * CHUNK + row]] + [o_recv[slot, k, row] for slot in range(GROUP - 1)]
                out_ref[k * CHUNK + row] = mix(factor, parts, i).astype(jnp.bfloat16)
            return carry

        return lax.fori_loop(0, CHUNK // tail - jnp.where(last, 1, 0), merge_piece, carry)

    lax.fori_loop(0, quarter, merge_chunk, 0)

    factor = factor_at(CHUNK // tail - 1)
    tail_factor[...] = factor
    for i in range(tail):
        row = kept + i
        base_ref[i] = mix(factor, [o_buf[(own_first + quarter - 1) * CHUNK + row], o_recv[SIBLING, quarter - 1, row]], i)
    wait_bytes(tail_ref, or_sem.at[quarter])
    wait_bytes(o_buf.at[pl.ds(0, (GROUP - 1) * quarter * CHUNK)], os_sem)
    wait_bytes(lse_buf.at[pl.ds(0, (GROUP - 1) * quarter)], ls_sem)

    @pl.when(core == 1)
    def _():
        send_handed().wait_send()


def solution(mesh):
    def local_step(q_blk, cache_blk, len_blk):
        rows, heads, width = q_blk.shape
        num_pages, page_len = cache_blk.shape[1], cache_blk.shape[3]
        cache_blk = jnp.swapaxes(cache_blk, 3, 4)
        latent = width - ROPE_DIM
        num_chunks = rows // CHUNK
        quarter = num_chunks // GROUP
        q_blk = jnp.transpose(q_blk, (1, 2, 0))
        dma = pltpu.SemaphoreType.DMA
        early_rows = rows // GROUP - PIECES[-1]
        tile = (GROUP * heads, latent)
        parts = pl.pallas_call(
            kernel,
            out_shape=(pltpu.VMEM((early_rows, *tile), jnp.bfloat16), pltpu.VMEM((2, PIECES[-1], *tile), jnp.bfloat16),
                       pltpu.VMEM((PIECES[-1], *tile), jnp.float32), pltpu.VMEM((GROUP * heads, 128), jnp.float32)),
            in_specs=[pl.BlockSpec(memory_space=pl.ANY), pl.BlockSpec(memory_space=pl.ANY),
                      pl.BlockSpec(memory_space=pl.ANY)],
            out_specs=(pl.BlockSpec(memory_space=pltpu.VMEM),) * 4,
            scratch_shapes=[
                pltpu.SMEM((rows,), jnp.int32),
                pltpu.VMEM((heads, latent, rows), jnp.bfloat16),
                pltpu.VMEM((heads, rows, latent), jnp.bfloat16),
                pltpu.VMEM((GROUP, rows, heads, latent), jnp.bfloat16),
                pltpu.VMEM((GROUP, heads, ROPE_DIM, rows), jnp.bfloat16),
                pltpu.VMEM((heads, rows, GROUP * ROPE_DIM), jnp.bfloat16),
                pltpu.VMEM((rows, heads, GROUP * ROPE_DIM), jnp.bfloat16),
                pltpu.VMEM((SLOTS, PAIR, num_pages, width, page_len), jnp.bfloat16),
                pltpu.VMEM((rows, GROUP * heads, latent), jnp.bfloat16),
                pltpu.VMEM((GROUP - 1, quarter, CHUNK, GROUP * heads, latent), jnp.bfloat16),
                pltpu.VMEM((num_chunks, CHUNK // 2, 128), jnp.float32),
                pltpu.VMEM((GROUP - 1, quarter, CHUNK // 2, 128), jnp.float32),
                pltpu.VMEM((128, 128), jnp.float32),
                pltpu.VMEM((PIECES[-1], GROUP * heads, latent), jnp.bfloat16),
                dma(()), dma((2,)), dma(()), dma((3,)), dma((SLOTS,)),
                dma(()), dma((num_chunks.bit_length(),)), dma(()), dma((num_chunks.bit_length(),)),
                dma(()), dma((quarter + len(PIECES) - 1,)), dma(()), dma((quarter,)), dma(()), dma(()),
                pltpu.SemaphoreType.REGULAR,
            ],
            compiler_params=pltpu.CompilerParams(collective_id=0, has_side_effects=True, vmem_limit_bytes=60 * 2**20),
        )(q_blk, cache_blk, len_blk)
        return pl.pallas_call(
            store,
            out_shape=jax.ShapeDtypeStruct((rows // GROUP, *tile), jnp.bfloat16),
            in_specs=[pl.BlockSpec(memory_space=pltpu.VMEM)] * 4,
            out_specs=pl.BlockSpec(memory_space=pl.ANY),
            scratch_shapes=[pltpu.VMEM((PIECES[-1], *tile), jnp.bfloat16), dma((2,))],
            compiler_params=pltpu.CompilerParams(vmem_limit_bytes=8 * 2**20),
        )(*[pltpu.with_memory_space_constraint(part, pltpu.VMEM) for part in parts])

    return jax.shard_map(local_step, mesh=mesh, in_specs=(P('dp', 'dcp', None), P('dp', None, 'dcp', None, None), P('dp')), out_specs=P(('dp', 'dcp'), None, None), check_vma=False)
```

```python
import functools
import math

import jax
import jax.numpy as jnp
from jax import lax
from jax.experimental import pallas as pl
from jax.experimental.pallas import tpu as pltpu
from jax.sharding import PartitionSpec as P

ROPE_DIM = 64
QK_DIM = 192
GROUP = 4
CHUNK = 16
PIECES = (12, 4)
PAIR = 2
SIBLING = 0
SLOTS = 2


def attend(q, q_rope, cache, base, length):
    num_pages, width, page_len = cache.shape
    latent = width - ROPE_DIM
    scores = []
    for j in range(num_pages):
        page = (jnp.dot(q, cache[j, :latent], preferred_element_type=jnp.float32)
                + jnp.dot(q_rope, cache[j, latent:], preferred_element_type=jnp.float32))
        if j >= num_pages // 2:
            lane = lax.broadcasted_iota(jnp.int32, (1, page_len), 1)
            page = jnp.where(lane < length - (j * GROUP + base) * page_len, page, -jnp.inf)
        scores.append(page)
    top = jnp.max(functools.reduce(jnp.maximum, scores), axis=1, keepdims=True)
    scale = QK_DIM**-0.5
    weights = [jnp.exp2((page - top) * (scale * math.log2(math.e))) for page in scores]
    total = jnp.sum(functools.reduce(jnp.add, weights), axis=1, keepdims=True)
    mixed = functools.reduce(jnp.add, [
        lax.dot_general(weights[j].astype(jnp.bfloat16), cache[j, :latent], (((1,), (1,)), ((), ())),
                        preferred_element_type=jnp.float32) for j in range(num_pages)])
    return (mixed / total).astype(jnp.bfloat16), top * scale + jnp.log(total)


def mix(factor, parts, i, first=0):
    half = CHUNK // 2
    return functools.reduce(jnp.add, [
        factor[:, n * half + i:n * half + i + 1] * part.astype(jnp.float32) for n, part in enumerate(parts, first)])


def store(early, tail, base, factor, out_hbm, buf, sems):
    done = early.shape[0]
    copies = [pltpu.make_async_copy(early, out_hbm.at[pl.ds(0, done)], sems.at[0]),
              pltpu.make_async_copy(buf, out_hbm.at[pl.ds(done, buf.shape[0])], sems.at[1])]
    copies[0].start()
    for i in range(buf.shape[0]):
        merged = base[i] + mix(factor[...], [tail[0, i]], i, 2) + mix(factor[...], [tail[1, i]], i, 3)
        buf[i] = merged.astype(jnp.bfloat16)
    copies[1].start()
    for copy in copies:
        copy.wait()


def kernel(q_hbm, cache_hbm, len_hbm, out_ref, tail_ref, base_ref, tail_factor, len_ref, q_raw, q_turned, q_all, rope_raw, rope_turned, rope_all, ring, o_buf, o_recv, lse_buf, lse_recv, factor_buf, stage,
           len_sem, own_sem, ps_sem, pr_sem, ring_sem, qs_sem, xr_sem, dr_sem, rr_sem, os_sem, or_sem, ls_sem, lr_sem, hs_sem, hr_sem, ready):
    heads, width, rows = q_hbm.shape
    latent = width - ROPE_DIM
    num_chunks = rows // CHUNK
    quarter = num_chunks // GROUP
    steps = rows // PAIR
    per_chunk = CHUNK // PAIR
    me = lax.axis_index("dcp")
    chip = me // 2
    core = me % 2
    across = (me + 2) % GROUP
    sibling = chip * 2 + (1 - core)
    diagonal = (sibling + 2) % GROUP
    first = (1 - chip) * (rows // 2)

    def start_row(k):
        return pl.multiple_of((first + k * CHUNK) % rows, CHUNK)

    def fetch(step):
        row = (first + step * PAIR) % rows
        slot = step % SLOTS
        return pltpu.make_async_copy(cache_hbm.at[pl.ds(row, PAIR), :, 0], ring.at[slot], ring_sem.at[slot])

    def send(src, dst, ssem, rsem, device):
        return pltpu.make_async_remote_copy(src_ref=src, dst_ref=dst, send_sem=ssem, recv_sem=rsem,
                                            device_id={"dcp": device}, device_id_type=pl.DeviceIdType.MESH)

    groups = [(0, 1)] + [(2**i, 2**i) for i in range(num_chunks.bit_length() - 1)]

    def rows_of(i, begin_at):
        start, size = groups[i]
        return pl.ds(pl.multiple_of((begin_at + start * CHUNK) % rows, CHUNK), size * CHUNK)

    def send_across(i):
        row = rows_of(i, chip * (rows // 2))
        return send(q_all.at[me, row], q_all.at[me, row], qs_sem, xr_sem.at[i], across)

    def got_across(i):
        row = rows_of(i, first)
        return send(q_all.at[me, row], q_all.at[across, row], qs_sem, xr_sem.at[i], across)

    def send_sibling():
        return send(q_all.at[me], q_all.at[me], qs_sem, dr_sem, sibling)

    def got_sibling():
        return send(q_all.at[me], q_all.at[sibling], qs_sem, dr_sem, sibling)

    def relay(i):
        row = rows_of(i, first)
        return send(q_all.at[across, row], q_all.at[across, row], qs_sem, rr_sem.at[i], sibling)

    def got_relay(i):
        row = rows_of(i, first)
        return send(q_all.at[across, row], q_all.at[diagonal, row], qs_sem, rr_sem.at[i], sibling)

    def wait_bytes(ref, semaphore):
        pltpu.make_async_copy(ref, ref, semaphore).wait()

    tail = PIECES[-1]
    kept = CHUNK - tail

    def send_part(g, slot, device, last):
        k = g % quarter
        split = last and slot is not SIBLING

        def part(begin, size, dst, semaphore):
            src = o_buf.at[pl.ds(pl.multiple_of(g * CHUNK + begin, math.gcd(begin, CHUNK)), size)]
            return send(src, dst, os_sem, semaphore, device)

        size = kept if split else CHUNK
        copies = [part(0, size, o_recv.at[slot, k, pl.ds(0, size)], or_sem.at[k]),
                  send(lse_buf.at[g], lse_recv.at[slot, k], ls_sem, lr_sem.at[k], device)]
        if split:
            copies.append(part(kept, tail, tail_ref.at[slot - 1], or_sem.at[quarter]))
        return copies

    crossing = 2 * quarter

    def hand_over():
        return send(o_buf.at[pl.ds(crossing * CHUNK - tail, tail)], stage, os_sem, hr_sem, sibling)

    def send_handed():
        return send(stage, tail_ref.at[1], hs_sem, or_sem.at[quarter], across)

    def start_part(g, slot, device):
        for last in (False, True):
            @pl.when((g % quarter == quarter - 1) == last)
            def _():
                copies = send_part(g, slot, device, last)
                for copy in copies[:2]:
                    copy.start()
                if len(copies) > 2:
                    handed = (g == crossing - 1) & (core == 0)

                    @pl.when(handed)
                    def _():
                        hand_over().start()

                    @pl.when(jnp.logical_not(handed))
                    def _():
                        copies[2].start()

    def send_rope(i, src, dst, device):
        return send(src, rope_raw.at[dst], ps_sem, pr_sem.at[i], device)

    def tell(semaphore, device):
        pl.semaphore_signal(semaphore, inc=1, device_id={"dcp": device}, device_id_type=pl.DeviceIdType.MESH)

    barrier = pltpu.get_barrier_semaphore()
    tell(barrier, across)

    own_rope = q_hbm.at[:, pl.ds(latent, ROPE_DIM), :]
    own = [pltpu.make_async_copy(q_hbm.at[:, pl.ds(0, latent), :], q_raw, own_sem.at[0]),
           pltpu.make_async_copy(own_rope, rope_raw.at[me], own_sem.at[1])]
    lengths = pltpu.make_async_copy(len_hbm, len_ref, len_sem)
    for copy in own + [lengths]:
        copy.start()
    for step in range(SLOTS - 1):
        fetch(step).start()

    pl.semaphore_wait(barrier, 3 - 2 * core)

    @pl.when(core == 1)
    def _():
        tell(barrier, sibling)
        tell(barrier, diagonal)

    @pl.when(core == 0)
    def _():
        tell(ready, sibling)
        tell(ready, diagonal)

    send_rope(0, own_rope, me, across).start()

    block = heads * heads
    into = lax.broadcasted_iota(jnp.int32, (block, block), 0)
    out_of = lax.broadcasted_iota(jnp.int32, (block, block), 1)
    swap = jnp.where(out_of == (into % heads) * heads + into // heads, 1.0, 0.0).astype(jnp.bfloat16)

    def interleave(turned, i):
        part = turned[:, pl.ds(pl.multiple_of(i * heads, heads), heads), :]
        lanes = part.shape[2]
        mixed = jnp.dot(swap, part.reshape(block, lanes), preferred_element_type=jnp.float32)
        return mixed.astype(jnp.bfloat16).reshape(heads, heads, lanes)

    own[0].wait()

    def turn(h, carry):
        q_turned[h] = q_raw[h].T
        return carry

    lax.fori_loop(0, heads, turn, 0)

    def place(i, carry):
        q_all[me, pl.ds(pl.multiple_of(i * heads, heads), heads)] = interleave(q_turned, i)
        return carry

    lax.fori_loop(0, rows // heads, place, 0)

    for i in range(len(groups)):
        send_across(i).start()

    @pl.when(core == 1)
    def _():
        pl.semaphore_wait(ready, 2)

    send_rope(1, own_rope, me, sibling).start()

    send_sibling().start()
    send_rope(0, own_rope, across, across).wait_recv()
    send_rope(2, rope_raw.at[across], across, sibling).start()
    own[1].wait()
    send_rope(1, own_rope, sibling, sibling).wait_recv()
    send_rope(2, rope_raw.at[across], diagonal, sibling).wait_recv()

    def turn_rope(h, carry):
        rope_turned[h] = jnp.concatenate(
            [jnp.concatenate([rope_raw[d, h], rope_raw[d + 1, h]], axis=0).T for d in range(0, GROUP, 2)], axis=1)
        return carry

    lax.fori_loop(0, heads, turn_rope, 0)

    def place_rope(i, carry):
        rope_all[pl.ds(pl.multiple_of(i * heads, heads), heads)] = interleave(rope_turned, i)
        return carry

    lax.fori_loop(0, rows // heads, place_rope, 0)
    got_across(0).wait_recv()
    relay(0).start()
    lengths.wait()
    got_sibling().wait_recv()

    def chunk_step(g, carry):
        for i, (start, _) in enumerate(groups):
            if i > 0:
                @pl.when(g + 1 == start)
                def _():
                    got_across(i).wait_recv()
                    relay(i).start()

            @pl.when(g == start)
            def _():
                got_relay(i).wait_recv()

        @pl.when((g == crossing + 1) & (core == 1))
        def _():
            hand_over().wait_recv()
            send_handed().start()

        def pair_step(p, lse_acc):
            step = g * per_chunk + p
            fetch(step).wait()

            @pl.when(step + SLOTS - 1 < steps)
            def _():
                fetch(step + SLOTS - 1).start()

            slot = step % SLOTS
            for i in range(PAIR):
                row = (first + step * PAIR + i) % rows
                q = jnp.concatenate([q_all[d, row] for d in range(GROUP)], axis=0)
                rope = rope_all[row]
                q_rope = jnp.concatenate([rope[:, d * ROPE_DIM:(d + 1) * ROPE_DIM] for d in range(GROUP)], axis=0)
                o, lse = attend(q, q_rope, ring[slot, i], me, len_ref[row])
                o_buf[step * PAIR + i] = o
                lane = lax.broadcasted_iota(jnp.int32, lse_acc.shape, 1)
                lse_acc = jnp.where(lane == p * PAIR + i, lse, lse_acc)
            return lse_acc

        lse_acc = lax.fori_loop(0, per_chunk, pair_step, jnp.zeros((GROUP * heads, 128), jnp.float32))
        columns = jnp.concatenate([lse_acc, lse_acc], axis=0).T
        half = CHUNK // 2
        left = lax.broadcasted_iota(jnp.int32, (half, 128), 1) < GROUP * heads
        lse_buf[g] = jnp.where(left, columns[:half], columns[half:CHUNK])

        @pl.when(g < 2 * quarter)
        def _():
            target = (1 - chip) * 2 + g // quarter
            start_part(g, 1 + (g // quarter + core) % 2, target)

        @pl.when((g >= 2 * quarter) & (g // quarter - 2 != core))
        def _():
            start_part(g, SIBLING, sibling)

        return carry

    lax.fori_loop(0, num_chunks, chunk_step, 0)

    own_first = (2 + core) * quarter

    wait_bytes(q_all.at[pl.ds(0, GROUP - 1)], qs_sem)
    wait_bytes(rope_raw.at[pl.ds(0, GROUP - 1)], ps_sem)

    half = CHUNK // 2
    every = GROUP * heads

    def factors_of(k):
        wait_bytes(lse_recv.at[:, k], lr_sem.at[k])
        lses = [lse_buf[own_first + k]] + [lse_recv[slot, k] for slot in range(GROUP - 1)]
        top = functools.reduce(jnp.maximum, lses)
        total = top + jnp.log(functools.reduce(jnp.add, [jnp.exp(x - top) for x in lses]))
        factors = jnp.concatenate([jnp.exp(x - total) for x in lses], axis=0)
        padded = jnp.concatenate([factors, jnp.zeros((128 - factors.shape[0], 128), jnp.float32)], axis=0)
        factor_buf[...] = padded.T

    def factor_at(m):
        factor = factor_buf[pl.ds(pl.multiple_of(m * tail // half * every, every), every)]
        return jnp.where(m * tail % half > 0, pltpu.roll(factor, 128 - tail, 1), factor)

    def merge_chunk(k, carry):
        last = k == quarter - 1
        factors_of(k)

        @pl.when(jnp.logical_not(last))
        def _():
            wait_bytes(o_buf.at[pl.ds(0, (GROUP - 1) * CHUNK)], or_sem.at[k])

        @pl.when(last)
        def _():
            wait_bytes(o_buf.at[pl.ds(0, (GROUP - 1) * CHUNK - 2 * tail)], or_sem.at[k])

        def merge_piece(m, carry):
            factor = factor_at(m)
            for i in range(tail):
                row = m * tail + i
                parts = [o_buf[(own_first + k) * CHUNK + row]] + [o_recv[slot, k, row] for slot in range(GROUP - 1)]
                out_ref[k * CHUNK + row] = mix(factor, parts, i).astype(jnp.bfloat16)
            return carry

        return lax.fori_loop(0, CHUNK // tail - jnp.where(last, 1, 0), merge_piece, carry)

    lax.fori_loop(0, quarter, merge_chunk, 0)

    factor = factor_at(CHUNK // tail - 1)
    tail_factor[...] = factor
    for i in range(tail):
        row = kept + i
        base_ref[i] = mix(factor, [o_buf[(own_first + quarter - 1) * CHUNK + row], o_recv[SIBLING, quarter - 1, row]], i)
    wait_bytes(tail_ref, or_sem.at[quarter])
    wait_bytes(o_buf.at[pl.ds(0, (GROUP - 1) * quarter * CHUNK)], os_sem)
    wait_bytes(lse_buf.at[pl.ds(0, (GROUP - 1) * quarter)], ls_sem)

    @pl.when(core == 1)
    def _():
        send_handed().wait_send()


def solution(mesh):
    def local_step(q_blk, cache_blk, len_blk):
        rows, heads, width = q_blk.shape
        num_pages, page_len = cache_blk.shape[1], cache_blk.shape[3]
        cache_blk = jnp.swapaxes(cache_blk, 3, 4)
        latent = width - ROPE_DIM
        num_chunks = rows // CHUNK
        quarter = num_chunks // GROUP
        q_blk = jnp.transpose(q_blk, (1, 2, 0))
        dma = pltpu.SemaphoreType.DMA
        early_rows = rows // GROUP - PIECES[-1]
        tile = (GROUP * heads, latent)
        parts = pl.pallas_call(
            kernel,
            out_shape=(pltpu.VMEM((early_rows, *tile), jnp.bfloat16), pltpu.VMEM((2, PIECES[-1], *tile), jnp.bfloat16),
                       pltpu.VMEM((PIECES[-1], *tile), jnp.float32), pltpu.VMEM((GROUP * heads, 128), jnp.float32)),
            in_specs=[pl.BlockSpec(memory_space=pl.ANY), pl.BlockSpec(memory_space=pl.ANY),
                      pl.BlockSpec(memory_space=pl.ANY)],
            out_specs=(pl.BlockSpec(memory_space=pltpu.VMEM),) * 4,
            scratch_shapes=[
                pltpu.SMEM((rows,), jnp.int32),
                pltpu.VMEM((heads, latent, rows), jnp.bfloat16),
                pltpu.VMEM((heads, rows, latent), jnp.bfloat16),
                pltpu.VMEM((GROUP, rows, heads, latent), jnp.bfloat16),
                pltpu.VMEM((GROUP, heads, ROPE_DIM, rows), jnp.bfloat16),
                pltpu.VMEM((heads, rows, GROUP * ROPE_DIM), jnp.bfloat16),
                pltpu.VMEM((rows, heads, GROUP * ROPE_DIM), jnp.bfloat16),
                pltpu.VMEM((SLOTS, PAIR, num_pages, width, page_len), jnp.bfloat16),
                pltpu.VMEM((rows, GROUP * heads, latent), jnp.bfloat16),
                pltpu.VMEM((GROUP - 1, quarter, CHUNK, GROUP * heads, latent), jnp.bfloat16),
                pltpu.VMEM((num_chunks, CHUNK // 2, 128), jnp.float32),
                pltpu.VMEM((GROUP - 1, quarter, CHUNK // 2, 128), jnp.float32),
                pltpu.VMEM((128, 128), jnp.float32),
                pltpu.VMEM((PIECES[-1], GROUP * heads, latent), jnp.bfloat16),
                dma(()), dma((2,)), dma(()), dma((3,)), dma((SLOTS,)),
                dma(()), dma((num_chunks.bit_length(),)), dma(()), dma((num_chunks.bit_length(),)),
                dma(()), dma((quarter + len(PIECES) - 1,)), dma(()), dma((quarter,)), dma(()), dma(()),
                pltpu.SemaphoreType.REGULAR,
            ],
            compiler_params=pltpu.CompilerParams(collective_id=0, has_side_effects=True, vmem_limit_bytes=60 * 2**20),
        )(q_blk, cache_blk, len_blk)
        return pl.pallas_call(
            store,
            out_shape=jax.ShapeDtypeStruct((rows // GROUP, *tile), jnp.bfloat16),
            in_specs=[pl.BlockSpec(memory_space=pltpu.VMEM)] * 4,
            out_specs=pl.BlockSpec(memory_space=pl.ANY),
            scratch_shapes=[pltpu.VMEM((PIECES[-1], *tile), jnp.bfloat16), dma((2,))],
            compiler_params=pltpu.CompilerParams(vmem_limit_bytes=8 * 2**20),
        )(*[pltpu.with_memory_space_constraint(part, pltpu.VMEM) for part in parts])

    return jax.shard_map(local_step, mesh=mesh, in_specs=(P('dp', 'dcp', None), P('dp', None, 'dcp', None, None), P('dp')), out_specs=P(('dp', 'dcp'), None, None), check_vma=False)
```
